256 devices in a mesh: seq: 4 (over y), lat: 32 (over x_hi, z, core), batch: 2 (over x_lo).
Axes of the slice: x: 4 (x_hi: 2, x_lo: 2; x = x_hi * 2 + x_lo), y: 4, z: 8, core: 2. Of those that a mesh axis runs over, the one named last changes fastest.
Arguments:
- activations: bfloat16 [2, 1024, 3584], P('batch', 'seq'), may hold values from -6 to 6
- dictionary: bfloat16 [32768, 3584], P('lat'), may hold values from -0.09375 to 0.09375
- topk_ids: int32 [2, 1024, 64], P('batch', 'seq'), may hold values from 0 to 32767, as said below
- kernel_taps: float32 [9, 32768], P(None, 'lat'), may hold values from -2 to 2
- enc_bias: float32 [32768], P('lat'), may hold values from -3 to 3
Outputs:
- grad_dictionary: float32 [32768, 3584], P('lat', ('seq', 'batch'))
- grad_taps: float32 [9, 32768], P(None, 'lat')
- grad_bias: float32 [32768], P('lat')
The draws below stay inside these ranges and needn't reach their ends.
Inputs may be any that keep to these rules, and one draw needn't show every extreme that they name: `topk_ids`: each position names 64 different latents.
All inputs are finite; a program needn't handle non-finite values.
Results may differ from the reference program's by a relative error of at most 0.017.
Values may be sent and summed in bfloat16 or wider, within the bound.
A program may use at most 128 MiB of HBM per device.

```python
import jax
import jax.numpy as jnp
from jax import lax

D = 3584
LAT_DEV = 1024
TOPK = 64
TAPS = 9
HALF = 4
LATENTS = 32768
LENGTH = 1024
SEQS = 2
N_SEQ = 4
N_LAT = 32


def draw_topk_ids(key, part):
    rows_all = SEQS * LENGTH
    spacing = LATENTS // TOPK
    row_order = jax.random.permutation(jax.random.fold_in(key, 11), rows_all).astype(jnp.int32)
    shifts = jax.random.randint(jax.random.fold_in(key, 12), (TOPK,), 0, spacing).astype(jnp.int32)
    latent_order = jax.random.permutation(jax.random.fold_in(key, 13), LATENTS).astype(jnp.int32)
    offsets = (row_order[:, None] + shifts[None, :]) % spacing
    slots = jnp.arange(TOPK, dtype=jnp.int32)[None, :] * spacing + offsets
    chosen = latent_order[slots]
    return chosen.reshape(SEQS, LENGTH, TOPK).astype(jnp.int32)


def strengthened(array, stream_key, source, target, shards_of, factor):
    def block_of(axis_at):
        return (jnp.arange(array.shape[axis_at]) // (array.shape[axis_at] // shards_of)).reshape((-1,) + (1,) * (array.ndim - 1 - axis_at))

    one_side = jax.random.permutation(stream_key, shards_of)[block_of(target)]
    other_side = (block_of(target) + shards_of // 2) % shards_of
    return jnp.where((block_of(source) == one_side) | (block_of(source) == other_side), factor * array, array)


def shard_levels(rng, shape, shards, smallest, largest):
    level, own = 1.0, jax.random.fold_in(rng, 6)
    for axis_at, blocks in shards:
        draws = jnp.exp(jax.random.uniform(jax.random.fold_in(own, axis_at), (blocks,), jnp.float32, smallest / len(shards), largest / len(shards)))
        level = level * jnp.repeat(draws, shape[axis_at] // blocks).reshape([-1 if axis == axis_at else 1 for axis in range(len(shape))])
    return level


def scatter_about(own_key, extent, scale, limit, shards=(), kind=jnp.bfloat16):
    array = jax.random.normal(own_key, extent, jnp.float32) * scale
    if len(shards) > 0:
        array = shard_levels(own_key, extent, shards, -0.22, 0.18) * array
    return jnp.clip(array, min=-limit, max=limit).astype(kind)


def heavy_noise(rng, extent, spread, bound, cuts, heavy, kind=jnp.bfloat16):
    drawn = spread * jax.random.normal(rng, extent, jnp.float32)
    if cuts:
        drawn = drawn * shard_levels(rng, extent, cuts, -0.22, 0.18)
    return jnp.clip(strengthened(drawn, jax.random.fold_in(rng, 3), *heavy), -bound, bound).astype(kind)


def setup_inputs(seed: int = 0) -> dict:
    splits = jax.random.split(jax.random.key(seed), 6)
    activations = heavy_noise(splits[0], (SEQS, LENGTH, D), 1.0, 6.0, ((0, 2), (1, 4)), (1, 2, 4, 2.0))
    dictionary = scatter_about(splits[1], (LATENTS, D), D ** -0.5, 0.09375, ((0, 32),))
    topk_ids = draw_topk_ids(jax.random.fold_in(splits[5], 71), 0)
    kernel_taps = scatter_about(splits[3], (TAPS, LATENTS), TAPS ** -0.5, 2.0, ((1, 32),), jnp.float32)
    enc_bias = scatter_about(splits[4], (LATENTS,), 0.5, 3.0, ((0, 32),), jnp.float32)
    return dict(activations=activations, dictionary=dictionary, topk_ids=topk_ids, kernel_taps=kernel_taps, enc_bias=enc_bias)


def lagged(field, taps_block, forward):
    length = field.shape[1]
    padded = jnp.pad(field, ((0, 0), (HALF, HALF), (0, 0)))
    summed = jnp.zeros(field.shape, jnp.float32)
    for tap_index in range(TAPS):
        begin = tap_index if forward else 2 * HALF - tap_index
        summed = summed + taps_block[tap_index][None, None, :] * padded[:, begin:begin + length, :]
    return summed


def block_codes(token_wide, dict_block, taps_block, bias_block, topk_ids, first):
    latent_in = jnp.einsum("std,ld->stl", token_wide, dict_block.astype(jnp.float32))
    preact = lagged(latent_in, taps_block, True) + bias_block[None, None, :]
    width_block = dict_block.shape[0]
    inside = (topk_ids >= first) & (topk_ids < first + width_block)
    local_ids = jnp.where(inside, topk_ids - first, width_block).astype(jnp.int32)
    seq_ids = jnp.arange(topk_ids.shape[0], dtype=jnp.int32)[:, None, None]
    pos_ids = jnp.arange(topk_ids.shape[1], dtype=jnp.int32)[None, :, None]
    active = jnp.zeros(latent_in.shape, jnp.float32).at[seq_ids, pos_ids, local_ids].set(1.0, mode="drop")
    latents = (active * preact).astype(jnp.bfloat16)
    return latent_in, active, latents


def reference(activations, dictionary, topk_ids, kernel_taps, enc_bias):
    seqs, length, width = activations.shape
    tok_block = length // N_SEQ
    token_wide = activations.astype(jnp.float32)
    dict_blocks = dictionary.reshape(N_LAT, LAT_DEV, width)
    taps_blocks = kernel_taps.reshape(TAPS, N_LAT, LAT_DEV).transpose(1, 0, 2)
    bias_blocks = enc_bias.reshape(N_LAT, LAT_DEV)
    firsts = jnp.arange(N_LAT, dtype=jnp.int32) * LAT_DEV
    items = (dict_blocks, taps_blocks, bias_blocks, firsts)

    def decode(carry, item):
        dict_block, taps_block, bias_block, first = item
        unused_in, unused_active, latents = block_codes(token_wide, dict_block, taps_block, bias_block, topk_ids, first)
        part = jnp.einsum("stl,ld->std", latents.astype(jnp.float32), dict_block.astype(jnp.float32))
        return carry + part, None

    recon, unused = lax.scan(decode, jnp.zeros(activations.shape, jnp.float32), items)
    residual = (recon - token_wide).astype(jnp.bfloat16)
    resid_wide = residual.astype(jnp.float32)
    resid_blocks = resid_wide.reshape(seqs, N_SEQ, tok_block, width)
    token_blocks = token_wide.reshape(seqs, N_SEQ, tok_block, width)

    def backward(item):
        dict_block, taps_block, bias_block, first = item
        latent_in, active, latents = block_codes(token_wide, dict_block, taps_block, bias_block, topk_ids, first)
        grad_code = jnp.einsum("std,ld->stl", resid_wide, dict_block.astype(jnp.float32))
        grad_pre = active * grad_code
        grad_in = lagged(grad_pre, taps_block, False).astype(jnp.bfloat16)
        padded_in = jnp.pad(latent_in, ((0, 0), (HALF, HALF), (0, 0)))
        tap_grads = jnp.stack([jnp.sum(grad_pre * padded_in[:, tap_index:tap_index + length, :], axis=(0, 1)) for tap_index in range(TAPS)])
        bias_grads = jnp.sum(grad_pre, axis=(0, 1))
        code_blocks = latents.astype(jnp.float32).reshape(seqs, N_SEQ, tok_block, -1)
        grad_blocks = grad_in.astype(jnp.float32).reshape(seqs, N_SEQ, tok_block, -1)
        terms = jnp.einsum("sjtl,sjtd->sjld", code_blocks, resid_blocks) + jnp.einsum("sjtl,sjtd->sjld", grad_blocks, token_blocks)
        rounded = lax.optimization_barrier(terms.astype(jnp.bfloat16)).astype(jnp.float32)
        return jnp.sum(rounded, axis=(0, 1)), tap_grads, bias_grads

    dict_grads, tap_grads, bias_grads = lax.map(backward, items)
    grad_dictionary = dict_grads.reshape(N_LAT * LAT_DEV, width)
    grad_taps = tap_grads.transpose(1, 0, 2).reshape(TAPS, N_LAT * LAT_DEV)
    grad_bias = bias_grads.reshape(N_LAT * LAT_DEV)
    return grad_dictionary, grad_taps, grad_bias
```

```python
import functools

import jax
import jax.numpy as jnp
from jax import lax
from jax.experimental import pallas as pl
from jax.experimental.pallas import tpu as pltpu
from jax.sharding import Mesh
from jax.sharding import PartitionSpec as P

TAPS = 9
HALF = 4
LAT = ("lat_0", "lat_1", "lat_2")
D = 3584
TOK = 256
LATS = 1024
SLOTS = 64
OWN = 448
GROUP = 8
NONE = 64
PIECES = 4
F32 = jnp.float32
BF16 = jnp.bfloat16
MESH = pl.DeviceIdType.MESH
VMEM = pl.BlockSpec(memory_space=pltpu.VMEM)
ANY = pl.BlockSpec(memory_space=pl.ANY)
BIG = 64 * 1024 * 1024 - 65536


def seat():
    return lax.axis_index("seq") * 2 + lax.axis_index("batch")


def peer(delta):
    j = lax.rem(seat() + delta, GROUP)
    return j, {"seq": j // 2, "batch": lax.rem(j, 2)}


def peer_from(delta):
    return lax.rem(seat() + GROUP - delta, GROUP)


def enter(partners):
    barrier = pltpu.get_barrier_semaphore()
    for device in partners:
        pl.semaphore_signal(barrier, inc=1, device_id=device, device_id_type=MESH)
    pl.semaphore_wait(barrier, len(partners))


def group_partners():
    return [peer(delta)[1] for delta in range(1, GROUP)]


def remote(src, dst, send_sem, recv_sem, device):
    return pltpu.make_async_remote_copy(
        src_ref=src,
        dst_ref=dst,
        send_sem=send_sem,
        recv_sem=recv_sem,
        device_id=device,
        device_id_type=MESH,
    )


def opening_kernel(
    act_ref, dict_ref, act8_ref, ids_ref,
    cols_ref, lat_ref, inv_ref, ids8_ref,
    dbuf, dsem, id_send, id_recv, act_send, act_recv, halo_send, halo_recv, own_sem,
):
    me = seat()
    seq = lax.axis_index("seq")
    for c in range(4):
        pltpu.make_async_copy(dict_ref.at[pl.ds(c * 256, 256)], dbuf.at[c], dsem.at[c]).start()
    enter(group_partners())
    sends = []
    for delta in range(1, GROUP):
        _, device = peer(delta)
        copy = remote(
            ids_ref, ids8_ref.at[me], id_send.at[delta - 1], id_recv.at[delta - 1], device
        )
        copy.start()
        sends.append(copy)
    for delta in range(1, GROUP):
        j, device = peer(delta)
        copy = remote(
            act8_ref.at[j], cols_ref.at[me], act_send.at[delta - 1], act_recv.at[delta - 1], device
        )
        copy.start()
        sends.append(copy)
    own_cols = pltpu.make_async_copy(act8_ref.at[me], cols_ref.at[me], own_sem.at[0])
    own_ids = pltpu.make_async_copy(ids_ref, ids8_ref.at[me], own_sem.at[1])
    own_cols.start()
    own_ids.start()

    def encode(c, carry):
        pltpu.make_async_copy(dict_ref.at[pl.ds(0, 256)], dbuf.at[c], dsem.at[c]).wait()
        lanes = pl.ds(pl.multiple_of(c * 256, 256), 256)
        lat_ref[8 : 8 + TOK, lanes] = lax.dot_general(
            act_ref[...], dbuf[c], (((1,), (1,)), ((), ())), preferred_element_type=F32
        )
        return carry

    lax.fori_loop(0, 4, encode, 0)
    left = {"seq": lax.rem(seq + 3, 4)}
    right = {"seq": lax.rem(seq + 1, 4)}
    to_left = remote(
        lat_ref.at[pl.ds(8, 8)], lat_ref.at[pl.ds(8 + TOK, 8)], halo_send.at[0], halo_recv.at[0], left
    )
    to_right = remote(
        lat_ref.at[pl.ds(TOK, 8)], lat_ref.at[pl.ds(0, 8)], halo_send.at[1], halo_recv.at[1], right
    )
    to_left.start()
    to_right.start()
    own_ids.wait()
    for delta in range(1, GROUP):
        pltpu.make_async_copy(ids_ref, ids8_ref.at[0], id_recv.at[delta - 1]).wait()

    first = (
        lax.axis_index("lat_0") * 16 + lax.axis_index("lat_1") * 2 + lax.axis_index("lat_2")
    ) * LATS
    lane = lax.broadcasted_iota(jnp.int32, (16, 128), 1).astype(F32).astype(BF16)

    def slot_rows(block, carry):
        j = block // 8
        row = pl.multiple_of(lax.rem(block, 8) * 16, 16)
        local = ids8_ref[j, pl.ds(row, 16), :] - first
        inside = (local >= 0) & (local < LATS)
        code = jnp.where(inside, local, 8 * 128)
        low = (code & 127).astype(F32).astype(BF16)
        high = (code >> 7).astype(F32).astype(BF16)
        for side in range(2):
            found = [jnp.full((16, 128), NONE, BF16) for _ in range(8)]
            for k in range(SLOTS):
                at = side * SLOTS + k
                here = lane == jnp.broadcast_to(low[:, at : at + 1], (16, 128))
                tile = jnp.where(
                    here, jnp.broadcast_to(high[:, at : at + 1], (16, 128)), jnp.array(8, BF16)
                )
                slot = jnp.array(k, BF16)
                for c in range(8):
                    found[c] = jnp.where(tile == jnp.array(c, BF16), slot, found[c])
            start = pl.multiple_of(j * TOK + side * 128 + row, 16)
            for c in range(8):
                inv_ref[pl.ds(start, 16), c * 128 : (c + 1) * 128] = found[c]
        return carry

    lax.fori_loop(0, 64, slot_rows, 0)

    to_left.wait()
    to_right.wait()
    lat_ref[0:8, :] = jnp.where(seq > 0, lat_ref[0:8, :], 0.0)
    lat_ref[8 + TOK :, :] = jnp.where(seq < 3, lat_ref[8 + TOK :, :], 0.0)
    own_cols.wait()
    for delta in range(1, GROUP):
        pltpu.make_async_copy(act8_ref.at[0], cols_ref.at[0], act_recv.at[delta - 1]).wait()
    for copy in sends:
        copy.wait_send()


def opening(act, dictionary, act8, ids):
    return pl.pallas_call(
        opening_kernel,
        out_shape=(
            jax.ShapeDtypeStruct((GROUP, TOK, OWN), BF16),
            jax.ShapeDtypeStruct((TOK + 16, LATS), F32),
            jax.ShapeDtypeStruct((GROUP * TOK, LATS), BF16),
            jax.ShapeDtypeStruct((GROUP, 128, 128), jnp.int32),
        ),
        in_specs=[VMEM, ANY, VMEM, VMEM],
        out_specs=(VMEM, VMEM, VMEM, VMEM),
        scratch_shapes=[
            pltpu.VMEM((4, 256, D), BF16),
            pltpu.SemaphoreType.DMA((4,)),
            pltpu.SemaphoreType.DMA((7,)),
            pltpu.SemaphoreType.DMA((7,)),
            pltpu.SemaphoreType.DMA((7,)),
            pltpu.SemaphoreType.DMA((7,)),
            pltpu.SemaphoreType.DMA((2,)),
            pltpu.SemaphoreType.DMA((2,)),
            pltpu.SemaphoreType.DMA((2,)),
        ],
        compiler_params=pltpu.CompilerParams(
            collective_id=0, has_side_effects=True, vmem_limit_bytes=48 * 1024 * 1024
        ),
        name="opening",
    )(act, dictionary, act8, ids)


def slots_of(read, ids, first):
    def rows(row):
        local = ids[pl.ds(row, 8), :] - first
        inside = (local >= 0) & (local < LATS)
        code = jnp.where(inside, local, 8 * 128)
        low, high = code & 127, code >> 7
        second = lax.broadcasted_iota(jnp.int32, (8, 128), 1) >= SLOTS
        total = jnp.zeros((8, 128), F32)
        for c in range(8):
            one = jnp.take_along_axis(read(row, c), low, axis=1)
            two = jnp.take_along_axis(read(row + 128, c), low, axis=1)
            total = jnp.where(high == c, jnp.where(second, two, one), total)
        return total

    return rows


def pick_kernel(first_ref, value_ref, ids_ref, out_ref):
    first = first_ref[0]

    def step(block, carry):
        row = pl.multiple_of(block * 16, 16)
        halves = []
        for part in range(2):
            at = pl.multiple_of(row + part * 8, 8)
            rows = slots_of(
                lambda r, c: value_ref[pl.ds(r, 8), c * 128 : (c + 1) * 128], ids_ref, first
            )
            halves.append(rows(at))
        out_ref[pl.ds(row, 16), :] = jnp.concatenate(halves, axis=0).astype(BF16)
        return carry

    lax.fori_loop(0, 8, step, 0)


def pick(first, values, ids):
    return pl.pallas_call(
        pick_kernel,
        out_shape=jax.ShapeDtypeStruct((128, 128), BF16),
        in_specs=[pl.BlockSpec(memory_space=pltpu.SMEM), VMEM, VMEM],
        out_specs=VMEM,
        name="pick",
    )(first, values, ids)


def sum_kernel(
    part_ref, act_ref, res8_ref,
    half, down_out, down_in, up_out, up_in, own_sum, other_sum, res, slices,
    half_sem, dsend, drecv, usend, urecv, xsend, xrecv, asend, arecv,
    gdsend, gdrecv, gusend, gurecv, csend, crecv, own_sem,
):
    me = seat()
    core = lax.axis_index("lat_2")
    z = lax.axis_index("lat_1")
    x = lax.axis_index("lat_0")
    other_core = {"lat_2": 1 - core}
    below = {"lat_1": lax.rem(z + 7, 8)}
    above = {"lat_1": lax.rem(z + 1, 8)}
    other_x = {"lat_0": 1 - x}
    enter([other_core, below, above, other_x] + group_partners())
    sends = []

    def start(copy):
        copy.start()
        sends.append(copy)

    give = pl.multiple_of((1 - core) * 128, 128)
    keep = pl.multiple_of(core * 128, 128)
    copy = remote(
        part_ref.at[pl.ds(give, 128)], half, half_sem.at[0], half_sem.at[1], other_core
    )
    start(copy)
    copy.wait_recv()
    width = D // PIECES

    def mine(chunk, h):
        cols = slice(h * width, (h + 1) * width)
        at = pl.multiple_of(chunk * 16, 16)
        return part_ref[pl.ds(keep + at, 16), cols].astype(F32) + half[pl.ds(at, 16), cols].astype(
            F32
        )

    for s in range(1, 6):
        for h in range(PIECES):
            cols = pl.ds(h * width, width)
            if s <= 4:
                value = mine(lax.rem(z + 8 - (5 - s), 8), h)
                if s > 1:
                    drecv_copy = pltpu.make_async_copy(
                        down_in.at[s - 2, :, cols], down_in.at[s - 2, :, cols], drecv.at[s - 2, h]
                    )
                    drecv_copy.wait()
                    value = value + down_in[s - 2, :, h * width : (h + 1) * width].astype(F32)
                down_out[s - 1, :, h * width : (h + 1) * width] = value.astype(BF16)
                start(
                    remote(
                        down_out.at[s - 1, :, cols],
                        down_in.at[s - 1, :, cols],
                        dsend.at[s - 1, h],
                        drecv.at[s - 1, h],
                        below,
                    )
                )
            if s <= 3:
                value = mine(lax.rem(z + (4 - s), 8), h)
                if s > 1:
                    pltpu.make_async_copy(
                        up_in.at[s - 2, :, cols], up_in.at[s - 2, :, cols], urecv.at[s - 2, h]
                    ).wait()
                    value = value + up_in[s - 2, :, h * width : (h + 1) * width].astype(F32)
                up_out[s - 1, :, h * width : (h + 1) * width] = value.astype(BF16)
                start(
                    remote(
                        up_out.at[s - 1, :, cols],
                        up_in.at[s - 1, :, cols],
                        usend.at[s - 1, h],
                        urecv.at[s - 1, h],
                        above,
                    )
                )
            if s == 5:
                pltpu.make_async_copy(
                    down_in.at[3, :, cols], down_in.at[3, :, cols], drecv.at[3, h]
                ).wait()
                pltpu.make_async_copy(
                    up_in.at[2, :, cols], up_in.at[2, :, cols], urecv.at[2, h]
                ).wait()
                at = slice(h * width, (h + 1) * width)
                total = mine(z, h) + down_in[3, :, at].astype(F32) + up_in[2, :, at].astype(F32)
                own_sum[:, at] = total.astype(BF16)
                start(
                    remote(
                        own_sum.at[:, cols],
                        other_sum.at[:, cols],
                        xsend.at[h],
                        xrecv.at[h],
                        other_x,
                    )
                )
    rows = pl.multiple_of(keep + z * 16, 16)
    for h in range(PIECES):
        cols = pl.ds(h * width, width)
        at = slice(h * width, (h + 1) * width)
        pltpu.make_async_copy(other_sum.at[:, cols], other_sum.at[:, cols], xrecv.at[h]).wait()
        res[:, at] = (own_sum[:, at].astype(F32) + other_sum[:, at].astype(F32)) - act_ref[
            pl.ds(rows, 16), at
        ].astype(F32)
    for j in range(GROUP):
        slices[j] = res[:, j * OWN : (j + 1) * OWN].astype(BF16)
    for delta in range(1, GROUP):
        j, device = peer(delta)
        start(
            remote(
                slices.at[j],
                res8_ref.at[me, pl.ds(rows, 16)],
                asend.at[delta - 1],
                arecv.at[delta - 1],
                device,
            )
        )
    own = pltpu.make_async_copy(slices.at[me], res8_ref.at[me, pl.ds(rows, 16)], own_sem)
    own.start()
    own.wait()
    for delta in range(1, GROUP):
        j = peer_from(delta)
        pltpu.make_async_copy(
            res8_ref.at[j, pl.ds(rows, 16)], res8_ref.at[j, pl.ds(rows, 16)], arecv.at[delta - 1]
        ).wait()

    def region(chunk, h):
        at = pl.multiple_of(keep + chunk * 16, 16)
        return res8_ref.at[pl.ds(h * 2, 2), pl.ds(at, 16)]

    def chunk_rows(base, chunk):
        at = pl.multiple_of(base + chunk * 16, 16)
        return res8_ref.at[:, pl.ds(at, 16)]

    def to_core(chunk, n):
        start(
            remote(
                chunk_rows(keep, chunk), chunk_rows(keep, chunk), csend.at[n], crecv.at[n], other_core
            )
        )

    for s in range(1, 6):
        for h in range(4):
            if s <= 4:
                chunk = lax.rem(z + s - 1, 8)
                if s > 1:
                    pltpu.make_async_copy(
                        region(chunk, h), region(chunk, h), gdrecv.at[s - 2, h]
                    ).wait()
                start(
                    remote(
                        region(chunk, h),
                        region(chunk, h),
                        gdsend.at[s - 1, h],
                        gdrecv.at[s - 1, h],
                        below,
                    )
                )
            else:
                chunk = lax.rem(z + 4, 8)
                pltpu.make_async_copy(region(chunk, h), region(chunk, h), gdrecv.at[3, h]).wait()
            if s <= 4:
                chunk = lax.rem(z + 8 - (s - 1), 8)
                if s > 1:
                    pltpu.make_async_copy(
                        region(chunk, h), region(chunk, h), gurecv.at[s - 2, h]
                    ).wait()
                if s <= 3:
                    start(
                        remote(
                            region(chunk, h),
                            region(chunk, h),
                            gusend.at[s - 1, h],
                            gurecv.at[s - 1, h],
                            above,
                        )
                    )
        to_core(lax.rem(z + s - 1, 8), s - 1)
        if 2 <= s <= 4:
            to_core(lax.rem(z + 8 - (s - 1), 8), 3 + s)
    for n in range(8):
        chunk = lax.rem(z + n, 8) if n < 5 else lax.rem(z + 8 - (n - 4), 8)
        there = pl.multiple_of(give, 128)
        pltpu.make_async_copy(
            chunk_rows(there, chunk), chunk_rows(there, chunk), crecv.at[n]
        ).wait()
    for copy in sends:
        copy.wait_send()


def summed(part, act):
    dma = pltpu.SemaphoreType.DMA
    return pl.pallas_call(
        sum_kernel,
        out_shape=jax.ShapeDtypeStruct((GROUP, TOK, OWN), BF16),
        in_specs=[VMEM, VMEM],
        out_specs=VMEM,
        scratch_shapes=[
            pltpu.VMEM((128, D), BF16),
            pltpu.VMEM((4, 16, D), BF16),
            pltpu.VMEM((4, 16, D), BF16),
            pltpu.VMEM((3, 16, D), BF16),
            pltpu.VMEM((3, 16, D), BF16),
            pltpu.VMEM((16, D), BF16),
            pltpu.VMEM((16, D), BF16),
            pltpu.VMEM((16, D), F32),
            pltpu.VMEM((GROUP, 16, OWN), BF16),
            dma((2,)),
            dma((4, PIECES)),
            dma((4, PIECES)),
            dma((3, PIECES)),
            dma((3, PIECES)),
            dma((PIECES,)),
            dma((PIECES,)),
            dma((7,)),
            dma((7,)),
            dma((4, 4)),
            dma((4, 4)),
            dma((3, 4)),
            dma((3, 4)),
            dma((8,)),
            dma((8,)),
            dma,
        ],
        compiler_params=pltpu.CompilerParams(
            collective_id=1, has_side_effects=True, vmem_limit_bytes=32 * 1024 * 1024
        ),
        name="summed",
    )(part, act)


def grads_kernel(first_ref, res_ref, dict_ref, ids_ref, out_ref, dense):
    first = first_ref[0]
    dense[...] = lax.dot_general(
        res_ref[0], dict_ref[...], (((1,), (1,)), ((), ())), preferred_element_type=F32
    )

    def step(block, carry):
        row = pl.multiple_of(block * 16, 16)
        halves = []
        for part in range(2):
            at = pl.multiple_of(row + part * 8, 8)
            rows = slots_of(
                lambda r, c: dense[pl.ds(r, 8), c * 128 : (c + 1) * 128], ids_ref.at[0], first
            )
            halves.append(rows(at))
        out_ref[0, pl.ds(row, 16), :] = jnp.concatenate(halves, axis=0).astype(BF16)
        return carry

    lax.fori_loop(0, 8, step, 0)


def grads(first, res8, dict_own, ids8):
    return pl.pallas_call(
        grads_kernel,
        grid=(GROUP,),
        out_shape=jax.ShapeDtypeStruct((GROUP, 128, 128), BF16),
        in_specs=[
            pl.BlockSpec(memory_space=pltpu.SMEM),
            pl.BlockSpec((1, TOK, OWN), lambda i: (i, 0, 0)),
            pl.BlockSpec((LATS, OWN), lambda i: (0, 0)),
            pl.BlockSpec((1, 128, 128), lambda i: (i, 0, 0)),
        ],
        out_specs=pl.BlockSpec((1, 128, 128), lambda i: (i, 0, 0)),
        scratch_shapes=[pltpu.VMEM((TOK, LATS), F32)],
        name="grads",
    )(first, res8, dict_own, ids8)


def codes_kernel(
    part_ref, codes_ref, total_ref, codes8_ref,
    arrived, own_total, psend, precv, csend, crecv, tsend, trecv, own_sem,
):
    me = seat()
    enter(group_partners())
    sends = []
    for delta in range(1, GROUP):
        j, device = peer(delta)
        copy = remote(
            part_ref.at[j], arrived.at[me], psend.at[delta - 1], precv.at[delta - 1], device
        )
        copy.start()
        sends.append(copy)
    for delta in range(1, GROUP):
        _, device = peer(delta)
        copy = remote(
            codes_ref, codes8_ref.at[me], csend.at[delta - 1], crecv.at[delta - 1], device
        )
        copy.start()
        sends.append(copy)
    own = pltpu.make_async_copy(part_ref.at[me], arrived.at[me], own_sem.at[0])
    own_codes = pltpu.make_async_copy(codes_ref, codes8_ref.at[me], own_sem.at[1])
    own.start()
    own_codes.start()
    own.wait()
    for delta in range(1, GROUP):
        pltpu.make_async_copy(part_ref.at[0], arrived.at[0], precv.at[delta - 1]).wait()
    total = arrived[0].astype(F32)
    for j in range(1, GROUP):
        total = total + arrived[j].astype(F32)
    own_total[...] = total.astype(BF16)
    for delta in range(1, GROUP):
        _, device = peer(delta)
        copy = remote(
            own_total, total_ref.at[me], tsend.at[delta - 1], trecv.at[delta - 1], device
        )
        copy.start()
        sends.append(copy)
    own_codes.wait()
    own = pltpu.make_async_copy(own_total, total_ref.at[me], own_sem.at[0])
    own.start()
    own.wait()
    for delta in range(1, GROUP):
        pltpu.make_async_copy(codes_ref, codes8_ref.at[0], crecv.at[delta - 1]).wait()
        pltpu.make_async_copy(own_total, total_ref.at[0], trecv.at[delta - 1]).wait()
    for copy in sends:
        copy.wait_send()


def all_codes(parts, codes):
    shape = jax.ShapeDtypeStruct((GROUP, 128, 128), BF16)
    return pl.pallas_call(
        codes_kernel,
        out_shape=(shape, shape),
        in_specs=[VMEM, VMEM],
        out_specs=(VMEM, VMEM),
        scratch_shapes=[
            pltpu.VMEM((GROUP, 128, 128), BF16),
            pltpu.VMEM((128, 128), BF16),
        ]
        + [pltpu.SemaphoreType.DMA((7,))] * 6
        + [pltpu.SemaphoreType.DMA((2,))],
        compiler_params=pltpu.CompilerParams(
            collective_id=2, has_side_effects=True, vmem_limit_bytes=16 * 1024 * 1024
        ),
        name="all_codes",
    )(parts, codes)


SEQ_ROWS = 4 * TOK + 16


def dictionary_kernel(
    where_ref, inv_ref, codes_ref, grad_ref, res_ref, act_ref, taps_ref, lat_ref,
    out_ref, small_ref, dense, pre, grad_in,
):
    width = inv_ref.shape[1]
    tiles = width // 128
    for b in range(2):
        pre[b, 0:8, :] = jnp.zeros((8, width), F32)
        pre[b, 8 + 4 * TOK :, :] = jnp.zeros((8, width), F32)
    keep = lax.broadcasted_iota(jnp.int32, (16, 128), 1) < SLOTS

    def expand(block, carry):
        j = block // 8
        row = pl.multiple_of(lax.rem(block, 8) * 16, 16)
        codes = codes_ref[j, pl.ds(row, 16), :].astype(F32)
        grad = grad_ref[j, pl.ds(row, 16), :].astype(F32)
        for side in range(2):
            if side:
                codes = pltpu.roll(codes, SLOTS, 1)
                grad = pltpu.roll(grad, SLOTS, 1)
            codes_side = jnp.where(keep, codes, 0.0)
            grad_side = jnp.where(keep, grad, 0.0)
            start = pl.multiple_of(j * TOK + side * 128 + row, 16)
            into = pl.multiple_of(8 + (j // 2) * TOK + side * 128 + row, 8)
            for c in range(tiles):
                at = slice(c * 128, (c + 1) * 128)
                slot = inv_ref[pl.ds(start, 16), at].astype(F32).astype(jnp.int32)
                wide = [
                    jnp.take_along_axis(codes_side[r : r + 8], slot[r : r + 8], axis=1)
                    for r in (0, 8)
                ]
                dense[pl.ds(start, 16), at] = jnp.concatenate(wide, axis=0).astype(BF16)
                for r in (0, 8):
                    pre[lax.rem(j, 2), pl.ds(into + r, 8), at] = jnp.take_along_axis(
                        grad_side[r : r + 8], slot[r : r + 8], axis=1
                    )
        return carry

    lax.fori_loop(0, 64, expand, 0)

    def spread(block, carry):
        b, row = block // 16, lax.rem(block, 16) * 64
        near = pre[b, pl.ds(pl.multiple_of(row, 8), 80), :]
        total = jnp.zeros((64, width), F32)
        for k in range(TAPS):
            begin = 8 + HALF - k
            total = total + taps_ref[k : k + 1, :] * near[begin : begin + 64]
        j = (row // TOK) * 2 + b
        into = pl.multiple_of(j * TOK + lax.rem(row, TOK), 64)
        grad_in[pl.ds(into, 64), :] = total.astype(BF16)
        return carry

    lax.fori_loop(0, 32, spread, 0)
    out_ref[...] = lax.dot_general(
        dense[...], res_ref[...], (((0,), (0,)), ((), ())), preferred_element_type=F32
    ) + lax.dot_general(
        grad_in[...], act_ref[...], (((0,), (0,)), ((), ())), preferred_element_type=F32
    )
    own = pre[where_ref[1], pl.ds(pl.multiple_of(8 + where_ref[0] * TOK, 8), TOK), :]
    for k in range(TAPS):
        small_ref[k : k + 1, :] = jnp.sum(
            own * lat_ref[k + HALF : k + HALF + TOK, :], axis=0, keepdims=True
        )
    small_ref[TAPS : TAPS + 1, :] = jnp.sum(own, axis=0, keepdims=True)
    small_ref[TAPS + 1 :, :] = jnp.zeros((16 - TAPS - 1, width), F32)


def dictionary_gradient(where, inv, codes8, grad8, res, cols, taps, lat):
    width = 256
    return pl.pallas_call(
        dictionary_kernel,
        grid=(LATS // width,),
        out_shape=(
            jax.ShapeDtypeStruct((LATS, OWN), F32),
            jax.ShapeDtypeStruct((16, LATS), F32),
        ),
        in_specs=[
            pl.BlockSpec(memory_space=pltpu.SMEM),
            pl.BlockSpec((GROUP * TOK, width), lambda i: (0, i)),
            pl.BlockSpec((GROUP, 128, 128), lambda i: (0, 0, 0)),
            pl.BlockSpec((GROUP, 128, 128), lambda i: (0, 0, 0)),
            pl.BlockSpec((GROUP * TOK, OWN), lambda i: (0, 0)),
            pl.BlockSpec((GROUP * TOK, OWN), lambda i: (0, 0)),
            pl.BlockSpec((TAPS, width), lambda i: (0, i)),
            pl.BlockSpec((TOK + 16, width), lambda i: (0, i)),
        ],
        out_specs=(
            pl.BlockSpec((width, OWN), lambda i: (i, 0)),
            pl.BlockSpec((16, width), lambda i: (0, i)),
        ),
        scratch_shapes=[
            pltpu.VMEM((GROUP * TOK, width), BF16),
            pltpu.VMEM((2, SEQ_ROWS, width), F32),
            pltpu.VMEM((GROUP * TOK, width), BF16),
        ],
        name="dictionary_gradient",
    )(where, inv, codes8, grad8, res, cols, taps, lat)


def small_kernel(part_ref, out_ref, arrived, send, recv):
    me = seat()
    enter(group_partners())
    sends = []
    for delta in range(1, GROUP):
        _, device = peer(delta)
        copy = remote(part_ref, arrived.at[me], send.at[delta - 1], recv.at[delta - 1], device)
        copy.start()
        sends.append(copy)
    arrived[me] = part_ref[...]
    for delta in range(1, GROUP):
        pltpu.make_async_copy(part_ref, arrived.at[0], recv.at[delta - 1]).wait()
    total = arrived[0]
    for j in range(1, GROUP):
        total = total + arrived[j]
    out_ref[...] = total
    for copy in sends:
        copy.wait_send()


def small_sum(part):
    return pl.pallas_call(
        small_kernel,
        out_shape=jax.ShapeDtypeStruct((16, LATS), F32),
        in_specs=[VMEM],
        out_specs=VMEM,
        scratch_shapes=[
            pltpu.VMEM((GROUP, 16, LATS), F32),
            pltpu.SemaphoreType.DMA((7,)),
            pltpu.SemaphoreType.DMA((7,)),
        ],
        compiler_params=pltpu.CompilerParams(
            collective_id=3, has_side_effects=True, vmem_limit_bytes=16 * 1024 * 1024
        ),
        name="small_sum",
    )(part)


def body(activations, dictionary, topk_ids, kernel_taps, enc_bias):
    act = activations[0]
    ids = topk_ids[0]
    ids = jnp.concatenate([ids[:128], ids[128:]], axis=1)
    me = seat()
    first = (lax.axis_index(LAT) * LATS).astype(jnp.int32)[None]
    act8 = act.reshape(TOK, GROUP, OWN).swapaxes(0, 1)
    cols, lat, inv, ids8 = opening(act, dictionary, act8, ids)
    preact = jnp.zeros((TOK, LATS), F32)
    for k in range(TAPS):
        preact = preact + kernel_taps[k][None, :] * lat[k + HALF : k + HALF + TOK]
    preact = preact + enc_bias[None, :]
    own_inv = lax.dynamic_slice_in_dim(inv, me * TOK, TOK, axis=0)
    latents = jnp.where(own_inv < NONE, preact, 0.0).astype(BF16)
    part = jnp.einsum("tl,ld->td", latents, dictionary, preferred_element_type=F32).astype(BF16)
    codes = pick(first, latents.astype(F32), ids)
    res8 = summed(part, act)
    dict_own = lax.dynamic_slice_in_dim(dictionary, me * OWN, OWN, axis=1)
    parts = grads(first, res8, dict_own, ids8)
    grad8, codes8 = all_codes(parts, codes)
    where = jnp.stack([lax.axis_index("seq"), lax.axis_index("batch")]).astype(jnp.int32)
    grad_dictionary, small = dictionary_gradient(
        where,
        inv,
        codes8,
        grad8,
        res8.reshape(GROUP * TOK, OWN),
        cols.reshape(GROUP * TOK, OWN),
        kernel_taps,
        lat,
    )
    small = small_sum(small)
    return grad_dictionary, small[:TAPS], small[TAPS]


def solution(mesh):
    finer = Mesh(
        mesh.devices.reshape(mesh.shape["seq"], 2, 8, 2, mesh.shape["batch"]),
        ("seq", "lat_0", "lat_1", "lat_2", "batch"),
    )
    return jax.shard_map(
        body,
        mesh=finer,
        in_specs=(
            P("batch", "seq", None),
            P(LAT, None),
            P("batch", "seq", None),
            P(None, LAT),
            P(LAT),
        ),
        out_specs=(P(LAT, ("seq", "batch")), P(None, LAT), P(LAT)),
        check_vma=False,
    )
```

```python
import functools

import jax
import jax.numpy as jnp
from jax import lax
from jax.experimental import pallas as pl
from jax.experimental.pallas import tpu as pltpu
from jax.sharding import Mesh
from jax.sharding import PartitionSpec as P

TAPS = 9
HALF = 4
LAT = ("lat_0", "lat_1", "lat_2")
D = 3584
TOK = 256
LATS = 1024
SLOTS = 64
OWN = 448
WIN = 512
GROUP = 8
NONE = 64
PIECES = 4
F32 = jnp.float32
BF16 = jnp.bfloat16
MESH = pl.DeviceIdType.MESH
VMEM = pl.BlockSpec(memory_space=pltpu.VMEM)
ANY = pl.BlockSpec(memory_space=pl.ANY)
BIG = 64 * 1024 * 1024 - 65536


def seat():
    return lax.axis_index("seq") * 2 + lax.axis_index("batch")


def peer(delta):
    j = lax.rem(seat() + delta, GROUP)
    return j, {"seq": j // 2, "batch": lax.rem(j, 2)}


def peer_from(delta):
    return lax.rem(seat() + GROUP - delta, GROUP)


def enter(partners):
    barrier = pltpu.get_barrier_semaphore()
    for device in partners:
        pl.semaphore_signal(barrier, inc=1, device_id=device, device_id_type=MESH)
    pl.semaphore_wait(barrier, len(partners))


def group_partners():
    return [peer(delta)[1] for delta in range(1, GROUP)]


def remote(src, dst, send_sem, recv_sem, device):
    return pltpu.make_async_remote_copy(
        src_ref=src,
        dst_ref=dst,
        send_sem=send_sem,
        recv_sem=recv_sem,
        device_id=device,
        device_id_type=MESH,
    )


def first_latent():
    group = lax.axis_index("lat_0") * 16 + lax.axis_index("lat_1") * 2 + lax.axis_index("lat_2")
    return group * LATS


def window(j):
    return pl.multiple_of((j * 7 // 2) * 128, 128)


def lanes_as_bf16():
    return lax.broadcasted_iota(jnp.int32, (16, 128), 1).astype(F32).astype(BF16)


def map_slots(ids, inv_ref, row, base, first):
    lane = lanes_as_bf16()
    local = ids[pl.ds(row, 16), :] - first
    inside = (local >= 0) & (local < LATS)
    code = jnp.where(inside, local, 8 * 128)
    low = (code & 127).astype(F32).astype(BF16)
    high = (code >> 7).astype(F32).astype(BF16)
    for side in range(2):
        found = [jnp.full((16, 128), NONE, BF16) for _ in range(8)]
        for k in range(SLOTS):
            at = side * SLOTS + k
            here = lane == jnp.broadcast_to(low[:, at : at + 1], (16, 128))
            tile = jnp.where(
                here, jnp.broadcast_to(high[:, at : at + 1], (16, 128)), jnp.array(8, BF16)
            )
            slot = jnp.array(k, BF16)
            for c in range(8):
                found[c] = jnp.where(tile == jnp.array(c, BF16), slot, found[c])
        start = pl.multiple_of(base + side * 128 + row, 16)
        for c in range(8):
            inv_ref[pl.ds(start, 16), c * 128 : (c + 1) * 128] = found[c]


def opening_kernel(
    act_ref, dict_ref, ids_ref, lat_ref, inv_ref, ids8_ref,
    dbuf, dsem, id_send, id_recv, halo_send, halo_recv, own_sem,
):
    me = seat()
    seq = lax.axis_index("seq")
    for c in range(4):
        pltpu.make_async_copy(dict_ref.at[pl.ds(c * 256, 256)], dbuf.at[c], dsem.at[c]).start()
    enter(group_partners())
    sends = []
    for delta in range(1, GROUP):
        _, device = peer(delta)
        copy = remote(
            ids_ref, ids8_ref.at[me], id_send.at[delta - 1], id_recv.at[delta - 1], device
        )
        copy.start()
        sends.append(copy)
    own_ids = pltpu.make_async_copy(ids_ref, ids8_ref.at[me], own_sem)
    own_ids.start()

    def encode(c, carry):
        pltpu.make_async_copy(dict_ref.at[pl.ds(0, 256)], dbuf.at[c], dsem.at[c]).wait()
        lanes = pl.ds(pl.multiple_of(c * 256, 256), 256)
        lat_ref[8 : 8 + TOK, lanes] = lax.dot_general(
            act_ref[...], dbuf[c], (((1,), (1,)), ((), ())), preferred_element_type=F32
        )
        return carry

    lax.fori_loop(0, 4, encode, 0)
    left = {"seq": lax.rem(seq + 3, 4)}
    right = {"seq": lax.rem(seq + 1, 4)}
    to_left = remote(
        lat_ref.at[pl.ds(8, 8)], lat_ref.at[pl.ds(8 + TOK, 8)], halo_send.at[0], halo_recv.at[0], left
    )
    to_right = remote(
        lat_ref.at[pl.ds(TOK, 8)], lat_ref.at[pl.ds(0, 8)], halo_send.at[1], halo_recv.at[1], right
    )
    to_left.start()
    to_right.start()

    def own_slots(block, carry):
        map_slots(ids_ref, inv_ref, pl.multiple_of(block * 16, 16), 0, first_latent())
        return carry

    lax.fori_loop(0, 8, own_slots, 0)
    own_ids.wait()
    for delta in range(1, GROUP):
        pltpu.make_async_copy(ids_ref, ids8_ref.at[0], id_recv.at[delta - 1]).wait()
    to_left.wait()
    to_right.wait()
    lat_ref[0:8, :] = jnp.where(seq > 0, lat_ref[0:8, :], 0.0)
    lat_ref[8 + TOK :, :] = jnp.where(seq < 3, lat_ref[8 + TOK :, :], 0.0)
    for copy in sends:
        copy.wait_send()


def opening(act, dictionary, ids):
    return pl.pallas_call(
        opening_kernel,
        out_shape=(
            jax.ShapeDtypeStruct((TOK + 16, LATS), F32),
            jax.ShapeDtypeStruct((TOK, LATS), BF16),
            jax.ShapeDtypeStruct((GROUP, 128, 128), jnp.int32),
        ),
        in_specs=[VMEM, ANY, VMEM],
        out_specs=(VMEM, VMEM, VMEM),
        scratch_shapes=[
            pltpu.VMEM((4, 256, D), BF16),
            pltpu.SemaphoreType.DMA((4,)),
            pltpu.SemaphoreType.DMA((7,)),
            pltpu.SemaphoreType.DMA((7,)),
            pltpu.SemaphoreType.DMA((2,)),
            pltpu.SemaphoreType.DMA((2,)),
            pltpu.SemaphoreType.DMA,
        ],
        compiler_params=pltpu.CompilerParams(
            collective_id=0, has_side_effects=True, vmem_limit_bytes=32 * 1024 * 1024
        ),
        name="opening",
    )(act, dictionary, ids)


def sum_kernel(
    part_ref, act_ref, ids8_ref, own_inv_ref, res8_ref, cols_ref, inv_ref,
    half, down_out, down_in, up_out, up_in, own_sum, other_sum, res, slices,
    half_sem, dsend, drecv, usend, urecv, xsend, xrecv, asend, arecv,
    gdsend, gdrecv, gusend, gurecv, csend, crecv, act_send, act_recv, own_sem,
):
    me = seat()
    core = lax.axis_index("lat_2")
    z = lax.axis_index("lat_1")
    x = lax.axis_index("lat_0")
    first = first_latent()
    other_core = {"lat_2": 1 - core}
    below = {"lat_1": lax.rem(z + 7, 8)}
    above = {"lat_1": lax.rem(z + 1, 8)}
    other_x = {"lat_0": 1 - x}
    give = pl.multiple_of((1 - core) * 128, 128)
    keep = pl.multiple_of(core * 128, 128)
    rows = pl.multiple_of(keep + z * 16, 16)

    def work(n):
        j = lax.rem(me + 1 + n // 8, GROUP)
        row = pl.multiple_of(lax.rem(n, 8) * 16, 16)
        map_slots(ids8_ref.at[j], inv_ref, row, j * TOK, first)

    def work_many(begin, end):
        def step(n, carry):
            work(n)
            return carry

        lax.fori_loop(begin, end, step, 0)

    own_inv = pltpu.make_async_copy(
        own_inv_ref, inv_ref.at[pl.ds(pl.multiple_of(me * TOK, TOK), TOK)], own_sem.at[0]
    )
    own_inv.start()
    own_cols = pltpu.make_async_copy(
        act_ref.at[:, pl.ds(window(me), WIN)], cols_ref.at[me], own_sem.at[1]
    )
    own_cols.start()
    enter([other_core, below, above, other_x] + group_partners())

    def half_copy():
        return remote(
            part_ref.at[pl.ds(give, 128)], half, half_sem.at[0], half_sem.at[1], other_core
        )

    def act_copy(delta):
        j, device = peer(delta)
        return remote(
            act_ref.at[:, pl.ds(window(j), WIN)],
            cols_ref.at[me],
            act_send.at[delta - 1],
            act_recv.at[delta - 1],
            device,
        )

    half_copy().start()
    for delta in range(1, GROUP):
        act_copy(delta).start()
    work_many(0, 3)
    half_copy().wait_recv()
    width = D // PIECES

    def cols_of(h):
        return pl.ds(pl.multiple_of(h * width, width), width)

    def mine(chunk, h):
        at = pl.multiple_of(chunk * 16, 16)
        return part_ref[pl.ds(keep + at, 16), cols_of(h)].astype(F32) + half[
            pl.ds(at, 16), cols_of(h)
        ].astype(F32)

    def down_copy(s, h):
        return remote(
            down_out.at[s, :, cols_of(h)],
            down_in.at[s, :, cols_of(h)],
            dsend.at[s, h],
            drecv.at[s, h],
            below,
        )

    def up_copy(s, h):
        return remote(
            up_out.at[s, :, cols_of(h)],
            up_in.at[s, :, cols_of(h)],
            usend.at[s, h],
            urecv.at[s, h],
            above,
        )

    def x_copy(h):
        return remote(
            own_sum.at[:, cols_of(h)], other_sum.at[:, cols_of(h)], xsend.at[h], xrecv.at[h], other_x
        )

    def far_sums(h, carry):
        down_out[0, :, cols_of(h)] = mine(lax.rem(z + 4, 8), h).astype(BF16)
        down_copy(0, h).start()
        up_out[0, :, cols_of(h)] = mine(lax.rem(z + 3, 8), h).astype(BF16)
        up_copy(0, h).start()
        return carry

    lax.fori_loop(0, PIECES, far_sums, 0)

    def near_sums(i, carry):
        s, h = i // PIECES + 1, lax.rem(i, PIECES)
        work(3 + i)
        down_copy(s - 1, h).wait_recv()
        down_out[s, :, cols_of(h)] = (
            mine(lax.rem(z + 4 + s, 8), h) + down_in[s - 1, :, cols_of(h)].astype(F32)
        ).astype(BF16)
        down_copy(s, h).start()

        @pl.when(s <= 2)
        def _():
            up_copy(s - 1, h).wait_recv()
            up_out[s, :, cols_of(h)] = (
                mine(lax.rem(z + 3 - s, 8), h) + up_in[s - 1, :, cols_of(h)].astype(F32)
            ).astype(BF16)
            up_copy(s, h).start()

        return carry

    lax.fori_loop(0, 3 * PIECES, near_sums, 0)

    def last_sums(h, carry):
        work(15 + h)
        down_copy(3, h).wait_recv()
        up_copy(2, h).wait_recv()
        total = mine(z, h) + down_in[3, :, cols_of(h)].astype(F32)
        total = total + up_in[2, :, cols_of(h)].astype(F32)
        own_sum[:, cols_of(h)] = total.astype(BF16)
        x_copy(h).start()
        return carry

    lax.fori_loop(0, PIECES, last_sums, 0)
    work_many(19, 23)
    for h in range(PIECES):
        x_copy(h).wait_recv()
    res[...] = (own_sum[...].astype(F32) + other_sum[...].astype(F32)) - act_ref[
        pl.ds(rows, 16), :
    ].astype(F32)
    for j in range(GROUP):
        begin = (j * 7 // 2) * 128
        column = lax.broadcasted_iota(jnp.int32, (16, WIN), 1) + begin
        owned = (column >= j * OWN) & (column < (j + 1) * OWN)
        slices[j] = jnp.where(owned, res[:, begin : begin + WIN], 0.0).astype(BF16)

    def slice_copy(delta):
        j, device = peer(delta)
        return remote(
            slices.at[j],
            res8_ref.at[me, pl.ds(rows, 16)],
            asend.at[delta - 1],
            arecv.at[delta - 1],
            device,
        )

    for delta in range(1, GROUP):
        slice_copy(delta).start()
    own = pltpu.make_async_copy(slices.at[me], res8_ref.at[me, pl.ds(rows, 16)], own_sem.at[2])
    own.start()
    work_many(23, 28)
    own.wait()
    for delta in range(1, GROUP):
        slice_copy(delta).wait_recv()

    def region(chunk, h):
        at = pl.multiple_of(keep + chunk * 16, 16)
        return res8_ref.at[pl.ds(h * 2, 2), pl.ds(at, 16)]

    def chunk_rows(base, chunk):
        at = pl.multiple_of(base + chunk * 16, 16)
        return res8_ref.at[:, pl.ds(at, 16)]

    def down_region(s, h):
        chunk = region(lax.rem(z + s, 8), h)
        return remote(chunk, chunk, gdsend.at[s, h], gdrecv.at[s, h], below)

    def up_region(s, h):
        chunk = region(lax.rem(z + 8 - s, 8), h)
        return remote(chunk, chunk, gusend.at[s, h], gurecv.at[s, h], above)

    def arrived(sem, chunk, h):
        pltpu.make_async_copy(region(chunk, h), region(chunk, h), sem).wait()

    def core_copy(chunk, n):
        part = chunk_rows(keep, chunk)
        return remote(part, part, csend.at[n], crecv.at[n], other_core)

    def first_regions(h, carry):
        down_region(0, h).start()
        up_region(0, h).start()
        return carry

    lax.fori_loop(0, 4, first_regions, 0)
    core_copy(z, 0).start()

    def next_regions(i, carry):
        s, h = i // 4 + 1, lax.rem(i, 4)
        work(28 + i)
        arrived(gdrecv.at[s - 1, h], lax.rem(z + s, 8), h)
        down_region(s, h).start()
        arrived(gurecv.at[s - 1, h], lax.rem(z + 8 - s, 8), h)

        @pl.when(s <= 2)
        def _():
            up_region(s, h).start()

        @pl.when(h == 3)
        def _():
            core_copy(lax.rem(z + s, 8), s).start()
            core_copy(lax.rem(z + 8 - s, 8), s + 4).start()

        return carry

    lax.fori_loop(0, 12, next_regions, 0)
    work_many(40, 44)
    for h in range(4):
        arrived(gdrecv.at[3, h], lax.rem(z + 4, 8), h)
    core_copy(lax.rem(z + 4, 8), 4).start()
    work_many(44, 56)
    for n in range(8):
        chunk = lax.rem(z + n, 8) if n < 5 else lax.rem(z + 12 - n, 8)
        part = chunk_rows(give, chunk)
        pltpu.make_async_copy(part, part, crecv.at[n]).wait()
    own_inv.wait()
    own_cols.wait()
    for delta in range(1, GROUP):
        act_copy(delta).wait_recv()
        act_copy(delta).wait_send()
        slice_copy(delta).wait_send()
    half_copy().wait_send()
    for h in range(PIECES):
        x_copy(h).wait_send()
    for n in range(8):
        core_copy(z, n).wait_send()

    def sent(i, carry):
        s, h = i // 4, lax.rem(i, 4)
        down_copy(s, h).wait_send()
        down_region(s, h).wait_send()

        @pl.when(s <= 2)
        def _():
            up_copy(s, h).wait_send()
            up_region(s, h).wait_send()

        return carry

    lax.fori_loop(0, 16, sent, 0)


def summed(part, act, ids8, own_inv):
    dma = pltpu.SemaphoreType.DMA
    return pl.pallas_call(
        sum_kernel,
        out_shape=(
            jax.ShapeDtypeStruct((GROUP, TOK, WIN), BF16),
            jax.ShapeDtypeStruct((GROUP, TOK, WIN), BF16),
            jax.ShapeDtypeStruct((GROUP * TOK, LATS), BF16),
        ),
        in_specs=[VMEM] * 4,
        out_specs=[VMEM] * 3,
        scratch_shapes=[
            pltpu.VMEM((128, D), BF16),
            pltpu.VMEM((4, 16, D), BF16),
            pltpu.VMEM((4, 16, D), BF16),
            pltpu.VMEM((3, 16, D), BF16),
            pltpu.VMEM((3, 16, D), BF16),
            pltpu.VMEM((16, D), BF16),
            pltpu.VMEM((16, D), BF16),
            pltpu.VMEM((16, D), F32),
            pltpu.VMEM((GROUP, 16, WIN), BF16),
            dma((2,)),
            dma((4, PIECES)),
            dma((4, PIECES)),
            dma((3, PIECES)),
            dma((3, PIECES)),
            dma((PIECES,)),
            dma((PIECES,)),
            dma((7,)),
            dma((7,)),
            dma((4, 4)),
            dma((4, 4)),
            dma((3, 4)),
            dma((3, 4)),
            dma((8,)),
            dma((8,)),
            dma((7,)),
            dma((7,)),
            dma((3,)),
        ],
        compiler_params=pltpu.CompilerParams(
            collective_id=1, has_side_effects=True, vmem_limit_bytes=40 * 1024 * 1024
        ),
        name="summed",
    )(part, act, ids8, own_inv)


def slots_of(read, ids, first):
    def rows(row):
        local = ids[pl.ds(row, 8), :] - first
        inside = (local >= 0) & (local < LATS)
        code = jnp.where(inside, local, 8 * 128)
        low, high = code & 127, code >> 7
        second = lax.broadcasted_iota(jnp.int32, (8, 128), 1) >= SLOTS
        total = jnp.zeros((8, 128), F32)
        for c in range(8):
            one = jnp.take_along_axis(read(row, c), low, axis=1)
            two = jnp.take_along_axis(read(row + 128, c), low, axis=1)
            total = jnp.where(high == c, jnp.where(second, two, one), total)
        return total

    return rows


def pick_slots(value_ref, ids, into, first):
    def step(block, carry):
        for part in range(2):
            row = pl.multiple_of(block * 32 + part * 16, 16)
            halves = []
            for side in range(2):
                at = pl.multiple_of(row + side * 8, 8)
                rows = slots_of(
                    lambda r, c: value_ref[pl.ds(r, 8), c * 128 : (c + 1) * 128], ids, first
                )
                halves.append(rows(at))
            into[pl.ds(row, 16), :] = jnp.concatenate(halves, axis=0).astype(BF16)
        return carry

    lax.fori_loop(0, 4, step, 0)


def codes_kernel(
    latents_ref, res8_ref, dict_ref, ids8_ref, inv_ref, lat_ref,
    total_ref, codes8_ref, small_ref,
    dwin, dense, codes, part, arrived, own_total, small_part, small_in,
    psend, precv, csend, crecv, tsend, trecv, ssend, srecv, own_sem,
):
    me = seat()
    first = first_latent()
    dict_copy = pltpu.make_async_copy(
        dict_ref.at[:, pl.ds(window(me), WIN)], dwin, own_sem.at[0]
    )
    dict_copy.start()
    dense[...] = latents_ref[...].astype(F32)
    pick_slots(dense, ids8_ref.at[me], codes, first)
    enter(group_partners())

    def code_copy(delta):
        return remote(
            codes, codes8_ref.at[me], csend.at[delta - 1], crecv.at[delta - 1], peer(delta)[1]
        )

    def part_copy(delta):
        j, device = peer(delta)
        return remote(part.at[j], arrived.at[me], psend.at[delta - 1], precv.at[delta - 1], device)

    def total_copy(delta):
        return remote(
            own_total, total_ref.at[me], tsend.at[delta - 1], trecv.at[delta - 1], peer(delta)[1]
        )

    def small_copy(delta):
        return remote(
            small_part, small_in.at[me], ssend.at[delta - 1], srecv.at[delta - 1], peer(delta)[1]
        )

    for delta in range(1, GROUP):
        code_copy(delta).start()
    dict_copy.wait()

    def block(n, carry):
        j = lax.rem(me + n, GROUP)
        dense[...] = lax.dot_general(
            res8_ref[j], dwin[...], (((1,), (1,)), ((), ())), preferred_element_type=F32
        )
        pick_slots(dense, ids8_ref.at[j], part.at[j], first)

        @pl.when(n < GROUP)
        def _():
            part_copy(n).start()

        return carry

    lax.fori_loop(1, GROUP + 1, block, 0)
    for delta in range(1, GROUP):
        part_copy(delta).wait_recv()
    arrived[me] = part[me]
    total = arrived[0].astype(F32)
    for j in range(1, GROUP):
        total = total + arrived[j].astype(F32)
    own_total[...] = total.astype(BF16)
    for delta in range(1, GROUP):
        total_copy(delta).start()
    keep = lax.broadcasted_iota(jnp.int32, (8, 128), 1) < SLOTS

    def expand(step, carry):
        row = pl.multiple_of(step * 16, 16)
        both = own_total[pl.ds(row, 16), :].astype(F32)
        for side in range(2):
            values = pltpu.roll(both, SLOTS, 1) if side else both
            at = pl.multiple_of(row + side * 128, 16)
            for c in range(8):
                lanes = slice(c * 128, (c + 1) * 128)
                slot = inv_ref[pl.ds(at, 16), lanes].astype(F32).astype(jnp.int32)
                for r in (0, 8):
                    dense[pl.ds(at + r, 8), lanes] = jnp.take_along_axis(
                        jnp.where(keep, values[r : r + 8], 0.0), slot[r : r + 8], axis=1
                    )
        return carry

    lax.fori_loop(0, 8, expand, 0)
    small_part[...] = jnp.zeros((16, LATS), F32)

    def correlate(c, carry):
        lanes = pl.ds(pl.multiple_of(c * 128, 128), 128)
        own = dense[:, lanes]
        wide = lat_ref[:, lanes]
        for k in range(TAPS):
            small_part[k : k + 1, lanes] = jnp.sum(
                own * wide[k + HALF : k + HALF + TOK], axis=0, keepdims=True
            )
        small_part[TAPS : TAPS + 1, lanes] = jnp.sum(own, axis=0, keepdims=True)
        return carry

    lax.fori_loop(0, 8, correlate, 0)
    for delta in range(1, GROUP):
        small_copy(delta).start()
    own_copies = [
        pltpu.make_async_copy(own_total, total_ref.at[me], own_sem.at[1]),
        pltpu.make_async_copy(codes, codes8_ref.at[me], own_sem.at[2]),
    ]
    for copy in own_copies:
        copy.start()
    small_in[me] = small_part[...]
    for copy in own_copies:
        copy.wait()
    for delta in range(1, GROUP):
        code_copy(delta).wait_recv()
        total_copy(delta).wait_recv()
        small_copy(delta).wait_recv()
    small = small_in[0]
    for j in range(1, GROUP):
        small = small + small_in[j]
    small_ref[...] = small
    for delta in range(1, GROUP):
        code_copy(delta).wait_send()
        part_copy(delta).wait_send()
        total_copy(delta).wait_send()
        small_copy(delta).wait_send()


def all_codes(latents, res8, dictionary, ids8, own_inv, lat):
    shape = jax.ShapeDtypeStruct((GROUP, 128, 128), BF16)
    dma = pltpu.SemaphoreType.DMA
    return pl.pallas_call(
        codes_kernel,
        out_shape=(shape, shape, jax.ShapeDtypeStruct((16, LATS), F32)),
        in_specs=[VMEM, VMEM, ANY, VMEM, VMEM, VMEM],
        out_specs=(VMEM, VMEM, VMEM),
        scratch_shapes=[
            pltpu.VMEM((LATS, WIN), BF16),
            pltpu.VMEM((TOK, LATS), F32),
            pltpu.VMEM((128, 128), BF16),
            pltpu.VMEM((GROUP, 128, 128), BF16),
            pltpu.VMEM((GROUP, 128, 128), BF16),
            pltpu.VMEM((128, 128), BF16),
            pltpu.VMEM((16, LATS), F32),
            pltpu.VMEM((GROUP, 16, LATS), F32),
        ]
        + [dma((7,))] * 8
        + [dma((3,))],
        compiler_params=pltpu.CompilerParams(
            collective_id=2, has_side_effects=True, vmem_limit_bytes=32 * 1024 * 1024
        ),
        name="all_codes",
    )(latents, res8, dictionary, ids8, own_inv, lat)


SEQ_ROWS = 4 * TOK + 16
UNROLL = 4


def dictionary_kernel(
    where_ref, inv_ref, codes_ref, grad_ref, res_ref, act_ref, taps_ref,
    out_ref, dense, pre, grad_in, res_t, act_t, product,
):
    width = inv_ref.shape[1]
    tiles = width // 128
    for c in range(tiles):
        for b in range(2):
            pre[c, b, 0:8, :] = jnp.zeros((8, 128), F32)
            pre[c, b, 8 + 4 * TOK :, :] = jnp.zeros((8, 128), F32)

    @pl.when(pl.program_id(0) == 0)
    def _():
        for j in range(GROUP):
            res_t[:, j * TOK : (j + 1) * TOK] = res_ref[j].T
            act_t[:, j * TOK : (j + 1) * TOK] = act_ref[j].T

    keep = lax.broadcasted_iota(jnp.int32, (16, 128), 1) < SLOTS

    def expand(block):
        j = block // 8
        row = pl.multiple_of(lax.rem(block, 8) * 16, 16)
        codes = codes_ref[j, pl.ds(row, 16), :].astype(F32)
        grad = grad_ref[j, pl.ds(row, 16), :].astype(F32)
        for side in range(2):
            if side:
                codes = pltpu.roll(codes, SLOTS, 1)
                grad = pltpu.roll(grad, SLOTS, 1)
            codes_side = jnp.where(keep, codes, 0.0)
            grad_side = jnp.where(keep, grad, 0.0)
            start = pl.multiple_of(j * TOK + side * 128 + row, 16)
            into = pl.multiple_of(8 + (j // 2) * TOK + side * 128 + row, 8)
            for c in range(tiles):
                at = slice(c * 128, (c + 1) * 128)
                slot = inv_ref[pl.ds(start, 16), at].astype(F32).astype(jnp.int32)
                wide = [
                    jnp.take_along_axis(codes_side[r : r + 8], slot[r : r + 8], axis=1)
                    for r in (0, 8)
                ]
                dense[pl.ds(start, 16), at] = jnp.concatenate(wide, axis=0).astype(BF16)
                for r in (0, 8):
                    pre[c, lax.rem(j, 2), pl.ds(into + r, 8), :] = jnp.take_along_axis(
                        grad_side[r : r + 8], slot[r : r + 8], axis=1
                    )

    def expand_some(step, carry):
        for u in range(UNROLL):
            expand(step * UNROLL + u)
        return carry

    lax.fori_loop(0, 64 // UNROLL, expand_some, 0)

    def spread(block, carry):
        b, row = block // 16, lax.rem(block, 16) * 64
        j = (row // TOK) * 2 + b
        into = pl.multiple_of(j * TOK + lax.rem(row, TOK), 64)
        for c in range(tiles):
            at = slice(c * 128, (c + 1) * 128)
            total = jnp.zeros((64, 128), F32)
            for k in range(TAPS):
                total = total + taps_ref[k : k + 1, at] * pre[c, b, pl.ds(row + (8 + HALF - k), 64), :]
            grad_in[pl.ds(into, 64), at] = total.astype(BF16)
        return carry

    lax.fori_loop(0, 32, spread, 0)
    product[...] = jnp.dot(
        res_t[...], dense[...], preferred_element_type=F32
    ) + jnp.dot(act_t[...], grad_in[...], preferred_element_type=F32)
    out_ref[...] = product[pl.ds(pl.multiple_of(where_ref[0], 64), OWN), :]


def dictionary_gradient(where, inv, codes8, grad8, res8, cols, taps):
    width = 256
    return pl.pallas_call(
        dictionary_kernel,
        grid=(LATS // width,),
        out_shape=jax.ShapeDtypeStruct((OWN, LATS), F32),
        in_specs=[
            pl.BlockSpec(memory_space=pltpu.SMEM),
            pl.BlockSpec((GROUP * TOK, width), lambda i: (0, i)),
            pl.BlockSpec((GROUP, 128, 128), lambda i: (0, 0, 0)),
            pl.BlockSpec((GROUP, 128, 128), lambda i: (0, 0, 0)),
            pl.BlockSpec((GROUP, TOK, WIN), lambda i: (0, 0, 0)),
            pl.BlockSpec((GROUP, TOK, WIN), lambda i: (0, 0, 0)),
            pl.BlockSpec((TAPS, width), lambda i: (0, i)),
        ],
        out_specs=pl.BlockSpec((OWN, width), lambda i: (0, i)),
        scratch_shapes=[
            pltpu.VMEM((GROUP * TOK, width), BF16),
            pltpu.VMEM((width // 128, 2, SEQ_ROWS, 128), F32),
            pltpu.VMEM((GROUP * TOK, width), BF16),
            pltpu.VMEM((WIN, GROUP * TOK), BF16),
            pltpu.VMEM((WIN, GROUP * TOK), BF16),
            pltpu.VMEM((WIN, width), F32),
        ],
        name="dictionary_gradient",
    )(where, inv, codes8, grad8, res8, cols, taps)


def body(activations, dictionary, topk_ids, kernel_taps, enc_bias):
    act = activations[0]
    ids = topk_ids[0]
    ids = jnp.concatenate([ids[:128], ids[128:]], axis=1)
    lat, own_inv, ids8 = opening(act, dictionary, ids)
    preact = jnp.zeros((TOK, LATS), F32)
    for k in range(TAPS):
        preact = preact + kernel_taps[k][None, :] * lat[k + HALF : k + HALF + TOK]
    preact = preact + enc_bias[None, :]
    latents = jnp.where(own_inv < NONE, preact, 0.0).astype(BF16)
    part = jnp.einsum("tl,ld->td", latents, dictionary, preferred_element_type=F32).astype(BF16)
    res8, cols, inv = summed(part, act, ids8, own_inv)
    grad8, codes8, small = all_codes(latents, res8, dictionary, ids8, own_inv, lat)
    where = (lax.axis_index("batch") * 64).astype(jnp.int32)[None]
    gradient = dictionary_gradient(where, inv, codes8, grad8, res8, cols, kernel_taps)
    return gradient.T, small[:TAPS], small[TAPS]


def solution(mesh):
    finer = Mesh(
        mesh.devices.reshape(mesh.shape["seq"], 2, 8, 2, mesh.shape["batch"]),
        ("seq", "lat_0", "lat_1", "lat_2", "batch"),
    )
    return jax.shard_map(
        body,
        mesh=finer,
        in_specs=(
            P("batch", "seq", None),
            P(LAT, None),
            P("batch", "seq", None),
            P(None, LAT),
            P(LAT),
        ),
        out_specs=(P(LAT, ("seq", "batch")), P(None, LAT), P(LAT)),
        check_vma=False,
    )
```

```python
import functools

import jax
import jax.numpy as jnp
from jax import lax
from jax.experimental import pallas as pl
from jax.experimental.pallas import tpu as pltpu
from jax.sharding import Mesh
from jax.sharding import PartitionSpec as P

TAPS = 9
HALF = 4
LAT = ("lat_0", "lat_1", "lat_2")
D = 3584
TOK = 256
LATS = 1024
SLOTS = 64
OWN = 448
WIN = 512
GROUP = 8
PIECES = 4
F32 = jnp.float32
BF16 = jnp.bfloat16
MESH = pl.DeviceIdType.MESH
VMEM = pl.BlockSpec(memory_space=pltpu.VMEM)
ANY = pl.BlockSpec(memory_space=pl.ANY)
OPENING_MIB = 50


def seat():
    return lax.axis_index("seq") * 2 + lax.axis_index("batch")


def peer(delta):
    j = lax.rem(seat() + delta, GROUP)
    return j, {"seq": j // 2, "batch": lax.rem(j, 2)}


def peer_from(delta):
    return lax.rem(seat() + GROUP - delta, GROUP)


def enter(partners):
    barrier = pltpu.get_barrier_semaphore()
    for device in partners:
        pl.semaphore_signal(barrier, inc=1, device_id=device, device_id_type=MESH)
    pl.semaphore_wait(barrier, len(partners))


def group_partners():
    return [peer(delta)[1] for delta in range(1, GROUP)]


def remote(src, dst, send_sem, recv_sem, device):
    return pltpu.make_async_remote_copy(
        src_ref=src,
        dst_ref=dst,
        send_sem=send_sem,
        recv_sem=recv_sem,
        device_id=device,
        device_id_type=MESH,
    )


def first_latent():
    group = lax.axis_index("lat_0") * 16 + lax.axis_index("lat_1") * 2 + lax.axis_index("lat_2")
    return group * LATS


def window(j):
    return pl.multiple_of((j * 7 // 2) * 128, 128)


def slot_rows(ids, side, first, rows_ref):
    code = ids[:, pl.ds(pl.multiple_of(side * 128, 128), 128)] - first
    inside = (code >= 0) & (code < LATS)
    hi = code >> 7
    part = hi & 3
    scale = jnp.where(
        part == 0, 1, jnp.where(part == 1, 1 << 7, jnp.where(part == 2, 1 << 14, 1 << 21))
    )
    value = (lax.broadcasted_iota(jnp.int32, (SLOTS, 128), 0) + SLOTS) * scale
    rows_ref[0] = jnp.where(inside, code & 127, -1)
    rows_ref[1] = jnp.where(inside & (hi < 4), value, 0)
    rows_ref[2] = jnp.where(inside & (hi >= 4), value, 0)


def slot_half(side, half, inv_ref, base, rows_ref, found_ref):
    sublane = lax.broadcasted_iota(jnp.int32, (8, 128), 0) + half * 64
    found = [[jnp.zeros((8, 128), jnp.int32) for _ in range(2)] for _ in range(8)]
    for k in range(SLOTS):
        low = jnp.broadcast_to(rows_ref[0, k : k + 1, :], (8, 128))
        values = [jnp.broadcast_to(rows_ref[1 + i, k : k + 1, :], (8, 128)) for i in range(2)]
        for r in range(8):
            here = low == sublane + r * 8
            for i in range(2):
                found[r][i] = found[r][i] + jnp.where(here, values[i], 0)
    for r in range(8):
        for i in range(2):
            found_ref[i, r * 8 : (r + 1) * 8, :] = found[r][i]
    into = pl.ds(pl.multiple_of(base + side * 128, 128), 128)
    for i in range(2):
        found_half = found_ref[i].T

        @pl.when(half == 0)
        def _():
            inv_ref[into, i * 128 : i * 128 + 64] = found_half

        @pl.when(half == 1)
        def _():
            inv_ref[into, i * 128 + 64 : (i + 1) * 128] = found_half


def map_slots(n, ids, inv_ref, base, first, rows_ref, found_ref):
    side, half = n // 2, lax.rem(n, 2)

    @pl.when(half == 0)
    def _():
        slot_rows(ids, side, first, rows_ref)

    slot_half(side, half, inv_ref, base, rows_ref, found_ref)


def slot_lane(packed, shift):
    return ((packed >> shift) + SLOTS) & 127


def opening_kernel(
    act_hbm, dict_ref, ids_hbm, taps_hbm, bias_hbm,
    latents_ref, part_ref, dwin_ref, lat_ref, inv_ref, ids8_ref,
    act_ref, dbuf, ids_ref, taps_ref, bias_ref, rows_ref, found_ref, dsem, id_send, id_recv, halo_send, halo_recv, own_sem,
):
    me = seat()
    seq = lax.axis_index("seq")
    ids_copy = pltpu.make_async_copy(ids_hbm, ids_ref, own_sem.at[2])
    act_copy = pltpu.make_async_copy(act_hbm, act_ref, own_sem.at[1])
    taps_copy = pltpu.make_async_copy(taps_hbm, taps_ref, own_sem.at[3])
    bias_copy = pltpu.make_async_copy(bias_hbm, bias_ref, own_sem.at[4])
    for copy in (ids_copy, act_copy):
        copy.start()
    for c in range(4):
        pltpu.make_async_copy(dict_ref.at[pl.ds(c * 256, 256)], dbuf.at[c], dsem.at[c]).start()
    for copy in (taps_copy, bias_copy):
        copy.start()
    enter(group_partners())
    ids_copy.wait()
    sends = []
    for delta in range(1, GROUP):
        _, device = peer(delta)
        copy = remote(
            ids_ref, ids8_ref.at[me], id_send.at[delta - 1], id_recv.at[delta - 1], device
        )
        copy.start()
        sends.append(copy)
    own_ids = pltpu.make_async_copy(ids_ref, ids8_ref.at[me], own_sem.at[0])
    own_ids.start()
    act_copy.wait()

    def encode(c, carry):
        pltpu.make_async_copy(dict_ref.at[pl.ds(0, 256)], dbuf.at[c], dsem.at[c]).wait()
        both = lax.dot_general(
            act_ref[...], dbuf[c], (((1,), (1,)), ((), ())), preferred_element_type=F32
        )
        lat_ref[2 * c, 8 : 8 + TOK, :] = both[:, :128]
        lat_ref[2 * c + 1, 8 : 8 + TOK, :] = both[:, 128:]
        return carry

    lax.fori_loop(0, 4, encode, 0)
    left = {"seq": lax.rem(seq + 3, 4)}
    right = {"seq": lax.rem(seq + 1, 4)}
    to_left = remote(
        lat_ref.at[:, pl.ds(8, 8)], lat_ref.at[:, pl.ds(8 + TOK, 8)],
        halo_send.at[0], halo_recv.at[0], left,
    )
    to_right = remote(
        lat_ref.at[:, pl.ds(TOK, 8)], lat_ref.at[:, pl.ds(0, 8)],
        halo_send.at[1], halo_recv.at[1], right,
    )
    to_left.start()
    to_right.start()
    dwin_ref[...] = dbuf[:, :, pl.ds(window(me), WIN)].reshape(LATS, WIN)

    def own_slots(n, carry):
        map_slots(n, ids_ref, inv_ref, 0, first_latent(), rows_ref, found_ref)
        return carry

    lax.fori_loop(0, 4, own_slots, 0)
    taps_copy.wait()
    bias_copy.wait()
    to_left.wait()
    to_right.wait()
    lat_ref[:, 0:8, :] = jnp.where(seq > 0, lat_ref[:, 0:8, :], 0.0)
    lat_ref[:, 8 + TOK :, :] = jnp.where(seq < 3, lat_ref[:, 8 + TOK :, :], 0.0)
    for c in range(8):
        at = slice(c * 128, (c + 1) * 128)
        total = jnp.zeros((TOK, 128), F32)
        for k in range(TAPS):
            total = total + taps_ref[k : k + 1, at] * lat_ref[c, k + HALF : k + HALF + TOK, :]
        total = total + bias_ref[:, at]
        packed = inv_ref[:, (c // 4) * 128 : (c // 4 + 1) * 128]
        active = ((packed >> (7 * (c % 4))) & 127) != 0
        latents_ref[:, at] = jnp.where(active, total, 0.0).astype(BF16)

    def decode(n, carry):
        at = pl.ds(pl.multiple_of(n * 512, 512), 512)
        part_ref[:, at] = jnp.dot(
            latents_ref[...], dbuf[:, :, at].reshape(LATS, 512), preferred_element_type=F32
        ).astype(BF16)
        return carry

    lax.fori_loop(0, D // 512, decode, 0)
    own_ids.wait()
    for delta in range(1, GROUP):
        pltpu.make_async_copy(ids_ref, ids8_ref.at[0], id_recv.at[delta - 1]).wait()
    for copy in sends:
        copy.wait_send()


SLOT_SCRATCH = [pltpu.VMEM((3, SLOTS, 128), jnp.int32), pltpu.VMEM((2, 64, 128), jnp.int32)]


def opening(act, dictionary, ids, taps, bias):
    return pl.pallas_call(
        opening_kernel,
        out_shape=(
            jax.ShapeDtypeStruct((TOK, LATS), BF16),
            jax.ShapeDtypeStruct((TOK, D), BF16),
            jax.ShapeDtypeStruct((LATS, WIN), BF16),
            jax.ShapeDtypeStruct((8, TOK + 16, 128), F32),
            jax.ShapeDtypeStruct((TOK, 256), jnp.int32),
            jax.ShapeDtypeStruct((GROUP, SLOTS, TOK), jnp.int32),
        ),
        in_specs=[ANY] * 5,
        out_specs=[VMEM] * 6,
        scratch_shapes=[
            pltpu.VMEM((TOK, D), BF16),
            pltpu.VMEM((4, 256, D), BF16),
            pltpu.VMEM((SLOTS, TOK), jnp.int32),
            pltpu.VMEM((TAPS, LATS), F32),
            pltpu.VMEM((1, LATS), F32),
            *SLOT_SCRATCH,
            pltpu.SemaphoreType.DMA((4,)),
            pltpu.SemaphoreType.DMA((7,)),
            pltpu.SemaphoreType.DMA((7,)),
            pltpu.SemaphoreType.DMA((2,)),
            pltpu.SemaphoreType.DMA((2,)),
            pltpu.SemaphoreType.DMA((5,)),
        ],
        compiler_params=pltpu.CompilerParams(
            collective_id=0, has_side_effects=True, vmem_limit_bytes=OPENING_MIB * 1024 * 1024
        ),
        name="opening",
    )(act, dictionary, ids, taps, bias)


def sum_kernel(
    part_ref, act_ref, ids8_ref, own_inv_ref, res8_ref, act_t_ref, inv_ref,
    cols_ref, rows_ref, found_ref, half, down_out, down_in, up_out, up_in, own_sum, other_sum, res, slices,
    half_sem, dsend, drecv, usend, urecv, xsend, xrecv, asend, arecv,
    gdsend, gdrecv, gusend, gurecv, csend, crecv, act_send, act_recv, swap_send, swap_recv, own_sem,
):
    me = seat()
    core = lax.axis_index("lat_2")
    z = lax.axis_index("lat_1")
    x = lax.axis_index("lat_0")
    first = first_latent()
    other_core = {"lat_2": 1 - core}
    below = {"lat_1": lax.rem(z + 7, 8)}
    above = {"lat_1": lax.rem(z + 1, 8)}
    other_x = {"lat_0": 1 - x}
    give = pl.multiple_of((1 - core) * 128, 128)
    keep = pl.multiple_of(core * 128, 128)
    rows = pl.multiple_of(keep + z * 16, 16)

    def work(n):
        j = lax.rem(me + 1 + n // 4, GROUP)
        map_slots(
            lax.rem(n, 4), ids8_ref.at[j], inv_ref, j * TOK, first, rows_ref, found_ref
        )

    def work_many(begin, end):
        def step(n, carry):
            work(n)
            return carry

        lax.fori_loop(begin, end, step, 0)

    own_inv = pltpu.make_async_copy(
        own_inv_ref, inv_ref.at[pl.ds(pl.multiple_of(me * TOK, TOK), TOK)], own_sem.at[0]
    )
    own_inv.start()
    own_cols = pltpu.make_async_copy(
        act_ref.at[:, pl.ds(window(me), WIN)], cols_ref.at[me], own_sem.at[1]
    )
    own_cols.start()
    enter([other_core, below, above, other_x] + group_partners())

    def half_copy():
        return remote(
            part_ref.at[pl.ds(give, 128)], half, half_sem.at[0], half_sem.at[1], other_core
        )

    def act_copy(delta):
        j, device = peer(delta)
        return remote(
            act_ref.at[pl.ds(keep, 128), pl.ds(window(j), WIN)],
            cols_ref.at[me, pl.ds(keep, 128)],
            act_send.at[delta - 1],
            act_recv.at[delta - 1],
            device,
        )

    def swap_copy(delta):
        rows_here = cols_ref.at[peer_from(delta), pl.ds(keep, 128)]
        return remote(
            rows_here, rows_here, swap_send.at[delta - 1], swap_recv.at[delta - 1], other_core
        )

    half_copy().start()
    for delta in range(1, GROUP):
        act_copy(delta).start()
    work_many(0, 3)
    half_copy().wait_recv()
    width = D // PIECES

    def cols_of(h):
        return pl.ds(pl.multiple_of(h * width, width), width)

    def mine(chunk, h):
        at = pl.multiple_of(chunk * 16, 16)
        return part_ref[pl.ds(keep + at, 16), cols_of(h)].astype(F32) + half[
            pl.ds(at, 16), cols_of(h)
        ].astype(F32)

    def down_copy(s, h):
        return remote(
            down_out.at[s, :, cols_of(h)],
            down_in.at[s, :, cols_of(h)],
            dsend.at[s, h],
            drecv.at[s, h],
            below,
        )

    def up_copy(s, h):
        return remote(
            up_out.at[s, :, cols_of(h)],
            up_in.at[s, :, cols_of(h)],
            usend.at[s, h],
            urecv.at[s, h],
            above,
        )

    def x_copy(h):
        return remote(
            own_sum.at[:, cols_of(h)], other_sum.at[:, cols_of(h)], xsend.at[h], xrecv.at[h], other_x
        )

    def far_sums(h, carry):
        down_out[0, :, cols_of(h)] = mine(lax.rem(z + 4, 8), h).astype(BF16)
        down_copy(0, h).start()
        up_out[0, :, cols_of(h)] = mine(lax.rem(z + 3, 8), h).astype(BF16)
        up_copy(0, h).start()
        return carry

    lax.fori_loop(0, PIECES, far_sums, 0)

    def near_sums(i, carry):
        s, h = i // PIECES + 1, lax.rem(i, PIECES)
        work(3 + i)
        down_copy(s - 1, h).wait_recv()
        down_out[s, :, cols_of(h)] = (
            mine(lax.rem(z + 4 + s, 8), h) + down_in[s - 1, :, cols_of(h)].astype(F32)
        ).astype(BF16)
        down_copy(s, h).start()

        @pl.when(s <= 2)
        def _():
            up_copy(s - 1, h).wait_recv()
            up_out[s, :, cols_of(h)] = (
                mine(lax.rem(z + 3 - s, 8), h) + up_in[s - 1, :, cols_of(h)].astype(F32)
            ).astype(BF16)
            up_copy(s, h).start()

        return carry

    lax.fori_loop(0, 3 * PIECES, near_sums, 0)

    def last_sums(h, carry):
        down_copy(3, h).wait_recv()
        up_copy(2, h).wait_recv()
        total = mine(z, h) + down_in[3, :, cols_of(h)].astype(F32)
        total = total + up_in[2, :, cols_of(h)].astype(F32)
        own_sum[:, cols_of(h)] = total.astype(BF16)
        x_copy(h).start()
        return carry

    lax.fori_loop(0, PIECES, last_sums, 0)
    work_many(15, 20)
    for h in range(PIECES):
        x_copy(h).wait_recv()
    res[...] = (own_sum[...].astype(F32) + other_sum[...].astype(F32)) - act_ref[
        pl.ds(rows, 16), :
    ].astype(F32)
    for j in range(GROUP):
        begin = (j * 7 // 2) * 128
        column = lax.broadcasted_iota(jnp.int32, (16, WIN), 1) + begin
        owned = (column >= j * OWN) & (column < (j + 1) * OWN)
        slices[j] = jnp.where(owned, res[:, begin : begin + WIN], 0.0).astype(BF16)

    def slice_copy(delta):
        j, device = peer(delta)
        return remote(
            slices.at[j],
            res8_ref.at[me, pl.ds(rows, 16)],
            asend.at[delta - 1],
            arecv.at[delta - 1],
            device,
        )

    for delta in range(1, GROUP):
        slice_copy(delta).start()
    own = pltpu.make_async_copy(slices.at[me], res8_ref.at[me, pl.ds(rows, 16)], own_sem.at[2])
    own.start()
    work_many(20, 24)
    for delta in range(1, GROUP):
        act_copy(delta).wait_recv()
        swap_copy(delta).start()
    own.wait()
    for delta in range(1, GROUP):
        slice_copy(delta).wait_recv()

    def region(chunk, h):
        at = pl.multiple_of(keep + chunk * 16, 16)
        return res8_ref.at[pl.ds(h * 2, 2), pl.ds(at, 16)]

    def chunk_rows(base, chunk):
        at = pl.multiple_of(base + chunk * 16, 16)
        return res8_ref.at[:, pl.ds(at, 16)]

    def down_region(s, h):
        chunk = region(lax.rem(z + s, 8), h)
        return remote(chunk, chunk, gdsend.at[s, h], gdrecv.at[s, h], below)

    def up_region(s, h):
        chunk = region(lax.rem(z + 8 - s, 8), h)
        return remote(chunk, chunk, gusend.at[s, h], gurecv.at[s, h], above)

    def arrived(sem, chunk, h):
        pltpu.make_async_copy(region(chunk, h), region(chunk, h), sem).wait()

    def core_copy(chunk, n):
        part = chunk_rows(keep, chunk)
        return remote(part, part, csend.at[n], crecv.at[n], other_core)

    def first_regions(h, carry):
        down_region(0, h).start()
        up_region(0, h).start()
        return carry

    lax.fori_loop(0, 4, first_regions, 0)
    core_copy(z, 0).start()

    def next_regions(i, carry):
        s, h = i // 4 + 1, lax.rem(i, 4)

        @pl.when(i < 4)
        def _():
            work(24 + i)

        @pl.when(i == 4)
        def _():
            own_cols.wait()

        @pl.when(i > 4)
        def _():
            swap_copy(i - 4).wait_recv()

        @pl.when(i >= 4)
        def _():
            j = lax.rem(me + 12 - i, GROUP)
            act_t_ref[:, pl.ds(pl.multiple_of(j * TOK, TOK), TOK)] = cols_ref[j].T

        arrived(gdrecv.at[s - 1, h], lax.rem(z + s, 8), h)
        down_region(s, h).start()
        arrived(gurecv.at[s - 1, h], lax.rem(z + 8 - s, 8), h)

        @pl.when(s <= 2)
        def _():
            up_region(s, h).start()

        @pl.when(h == 3)
        def _():
            core_copy(lax.rem(z + s, 8), s).start()
            core_copy(lax.rem(z + 8 - s, 8), s + 4).start()

        return carry

    lax.fori_loop(0, 12, next_regions, 0)
    for h in range(4):
        arrived(gdrecv.at[3, h], lax.rem(z + 4, 8), h)
    core_copy(lax.rem(z + 4, 8), 4).start()
    for n in range(8):
        chunk = lax.rem(z + n, 8) if n < 5 else lax.rem(z + 12 - n, 8)
        part = chunk_rows(give, chunk)
        pltpu.make_async_copy(part, part, crecv.at[n]).wait()
    own_inv.wait()
    for delta in range(1, GROUP):
        act_copy(delta).wait_send()
        swap_copy(delta).wait_send()
        slice_copy(delta).wait_send()
    half_copy().wait_send()
    for h in range(PIECES):
        x_copy(h).wait_send()
    for n in range(8):
        core_copy(z, n).wait_send()

    def sent(i, carry):
        s, h = i // 4, lax.rem(i, 4)
        down_copy(s, h).wait_send()
        down_region(s, h).wait_send()

        @pl.when(s <= 2)
        def _():
            up_copy(s, h).wait_send()
            up_region(s, h).wait_send()

        return carry

    lax.fori_loop(0, 16, sent, 0)


def summed(part, act, ids8, own_inv):
    dma = pltpu.SemaphoreType.DMA
    return pl.pallas_call(
        sum_kernel,
        out_shape=(
            jax.ShapeDtypeStruct((GROUP, TOK, WIN), BF16),
            jax.ShapeDtypeStruct((WIN, GROUP * TOK), BF16),
            jax.ShapeDtypeStruct((GROUP * TOK, 256), jnp.int32),
        ),
        in_specs=[VMEM] * 4,
        out_specs=[VMEM] * 3,
        scratch_shapes=[
            pltpu.VMEM((GROUP, TOK, WIN), BF16),
            *SLOT_SCRATCH,
            pltpu.VMEM((128, D), BF16),
            pltpu.VMEM((4, 16, D), BF16),
            pltpu.VMEM((4, 16, D), BF16),
            pltpu.VMEM((3, 16, D), BF16),
            pltpu.VMEM((3, 16, D), BF16),
            pltpu.VMEM((16, D), BF16),
            pltpu.VMEM((16, D), BF16),
            pltpu.VMEM((16, D), F32),
            pltpu.VMEM((GROUP, 16, WIN), BF16),
            dma((2,)),
            dma((4, PIECES)),
            dma((4, PIECES)),
            dma((3, PIECES)),
            dma((3, PIECES)),
            dma((PIECES,)),
            dma((PIECES,)),
            dma((7,)),
            dma((7,)),
            dma((4, 4)),
            dma((4, 4)),
            dma((3, 4)),
            dma((3, 4)),
            dma((8,)),
            dma((8,)),
            dma((7,)),
            dma((7,)),
            dma((7,)),
            dma((7,)),
            dma((3,)),
        ],
        compiler_params=pltpu.CompilerParams(
            collective_id=1, has_side_effects=True, vmem_limit_bytes=24 * 1024 * 1024
        ),
        name="summed",
    )(part, act, ids8, own_inv)


def slots_of(read, ids, first):
    def rows(row):
        local = ids[pl.ds(row, 8), :] - first
        inside = (local >= 0) & (local < LATS)
        code = jnp.where(inside, local, 8 * 128)
        low, high = code & 127, code >> 7
        second = lax.broadcasted_iota(jnp.int32, (8, 128), 1) >= SLOTS
        total = jnp.zeros((8, 128), F32)
        for c in range(8):
            one = jnp.take_along_axis(read(row, c), low, axis=1)
            two = jnp.take_along_axis(read(row + 128, c), low, axis=1)
            total = jnp.where(high == c, jnp.where(second, two, one), total)
        return total

    return rows


def pick_slots(value_ref, ids, into, first):
    def step(block, carry):
        for part in range(2):
            row = pl.multiple_of(block * 32 + part * 16, 16)
            halves = []
            for side in range(2):
                at = pl.multiple_of(row + side * 8, 8)
                rows = slots_of(
                    lambda r, c: value_ref[pl.ds(r, 8), c * 128 : (c + 1) * 128], ids, first
                )
                halves.append(rows(at))
            into[pl.ds(row, 16), :] = jnp.concatenate(halves, axis=0).astype(BF16)
        return carry

    lax.fori_loop(0, 4, step, 0)


def codes_kernel(
    latents_ref, res8_ref, dwin, ids8_ref, inv_ref, lat_ref,
    total_ref, codes8_ref, small_ref,
    dense, ids_rows, codes, part, arrived, own_total, small_part, small_out, small_in,
    psend, precv, csend, crecv, tsend, trecv, ssend, srecv, own_sem,
):
    me = seat()
    first = first_latent()
    dense[...] = latents_ref[...].astype(F32)

    def rows_of(j):
        ids = ids8_ref[j]
        ids_rows[...] = jnp.concatenate([ids[:, :128], ids[:, 128:]], axis=0).T

    rows_of(me)
    pick_slots(dense, ids_rows, codes, first)
    enter(group_partners())

    def code_copy(delta):
        return remote(
            codes, codes8_ref.at[me], csend.at[delta - 1], crecv.at[delta - 1], peer(delta)[1]
        )

    def part_copy(delta):
        j, device = peer(delta)
        return remote(part.at[j], arrived.at[me], psend.at[delta - 1], precv.at[delta - 1], device)

    def total_copy(delta):
        return remote(
            own_total, total_ref.at[me], tsend.at[delta - 1], trecv.at[delta - 1], peer(delta)[1]
        )

    def small_copy(delta):
        return remote(
            small_out, small_in.at[me], ssend.at[delta - 1], srecv.at[delta - 1], peer(delta)[1]
        )

    for delta in range(1, GROUP):
        code_copy(delta).start()

    def block(n, carry):
        j = lax.rem(me + n, GROUP)
        dense[...] = lax.dot_general(
            res8_ref[j], dwin[...], (((1,), (1,)), ((), ())), preferred_element_type=F32
        )
        rows_of(j)
        pick_slots(dense, ids_rows, part.at[j], first)

        @pl.when(n < GROUP)
        def _():
            part_copy(n).start()

        return carry

    lax.fori_loop(1, GROUP + 1, block, 0)
    for delta in range(1, GROUP):
        part_copy(delta).wait_recv()
    arrived[me] = part[me]
    total = arrived[0].astype(F32)
    for j in range(1, GROUP):
        total = total + arrived[j].astype(F32)
    own_total[...] = total.astype(BF16)
    for delta in range(1, GROUP):
        total_copy(delta).start()
    keep = lax.broadcasted_iota(jnp.int32, (8, 128), 1) < SLOTS

    def expand(step, carry):
        row = pl.multiple_of(step * 16, 16)
        both = own_total[pl.ds(row, 16), :].astype(F32)
        for side in range(2):
            values = pltpu.roll(both, SLOTS, 1) if side else both
            at = pl.multiple_of(row + side * 128, 16)
            for c in range(8):
                lanes = slice(c * 128, (c + 1) * 128)
                packed = inv_ref[pl.ds(at, 16), (c // 4) * 128 : (c // 4 + 1) * 128]
                slot = slot_lane(packed, 7 * (c % 4))
                for r in (0, 8):
                    dense[pl.ds(at + r, 8), lanes] = jnp.take_along_axis(
                        jnp.where(keep, values[r : r + 8], 0.0), slot[r : r + 8], axis=1
                    )
        return carry

    lax.fori_loop(0, 8, expand, 0)
    small_part[TAPS + 1 :, :] = jnp.zeros((16 - TAPS - 1, LATS), F32)

    def correlate(c, carry):
        lanes = pl.ds(pl.multiple_of(c * 128, 128), 128)
        own = dense[:, lanes]
        for k in range(TAPS):
            small_part[k : k + 1, lanes] = jnp.sum(
                own * lat_ref[c, k + HALF : k + HALF + TOK, :], axis=0, keepdims=True
            )
        small_part[TAPS : TAPS + 1, lanes] = jnp.sum(own, axis=0, keepdims=True)
        return carry

    lax.fori_loop(0, 8, correlate, 0)
    small_out[...] = small_part[...].astype(BF16)
    for delta in range(1, GROUP):
        small_copy(delta).start()
    own_copies = [
        pltpu.make_async_copy(own_total, total_ref.at[me], own_sem.at[1]),
        pltpu.make_async_copy(codes, codes8_ref.at[me], own_sem.at[2]),
    ]
    for copy in own_copies:
        copy.start()
    small_in[me] = small_out[...]
    for copy in own_copies:
        copy.wait()
    for delta in range(1, GROUP):
        code_copy(delta).wait_recv()
        total_copy(delta).wait_recv()
        small_copy(delta).wait_recv()
    small = small_in[0].astype(F32)
    for j in range(1, GROUP):
        small = small + small_in[j].astype(F32)
    small_ref[...] = small
    for delta in range(1, GROUP):
        code_copy(delta).wait_send()
        part_copy(delta).wait_send()
        total_copy(delta).wait_send()
        small_copy(delta).wait_send()


def all_codes(latents, res8, dwin, ids8, own_inv, lat):
    shape = jax.ShapeDtypeStruct((GROUP, 128, 128), BF16)
    dma = pltpu.SemaphoreType.DMA
    return pl.pallas_call(
        codes_kernel,
        out_shape=(shape, shape, jax.ShapeDtypeStruct((16, LATS), F32)),
        in_specs=[VMEM] * 6,
        out_specs=(VMEM, VMEM, VMEM),
        scratch_shapes=[
            pltpu.VMEM((TOK, LATS), F32),
            pltpu.VMEM((128, 128), jnp.int32),
            pltpu.VMEM((128, 128), BF16),
            pltpu.VMEM((GROUP, 128, 128), BF16),
            pltpu.VMEM((GROUP, 128, 128), BF16),
            pltpu.VMEM((128, 128), BF16),
            pltpu.VMEM((16, LATS), F32),
            pltpu.VMEM((16, LATS), BF16),
            pltpu.VMEM((GROUP, 16, LATS), BF16),
        ]
        + [dma((7,))] * 8
        + [dma((3,))],
        compiler_params=pltpu.CompilerParams(
            collective_id=2, has_side_effects=True, vmem_limit_bytes=16 * 1024 * 1024
        ),
        name="all_codes",
    )(latents, res8, dwin, ids8, own_inv, lat)


SEQ_ROWS = 4 * TOK + 16
CHUNK = 256


def dictionary_kernel(
    where_ref, inv_hbm, codes_hbm, grad_hbm, res_hbm, act_t_hbm, taps_ref,
    out_ref, inv_ref, codes_ref, grad_ref, res_ref, act_t_ref, dense, pre, grad_in, res_t, product, sems,
):
    sources = [inv_hbm, codes_hbm, grad_hbm, res_hbm, act_t_hbm]
    targets = [inv_ref, codes_ref, grad_ref, res_ref, act_t_ref]
    copies = [pltpu.make_async_copy(a, b, sems.at[n]) for n, (a, b) in enumerate(zip(sources, targets))]
    for n in (1, 2, 0, 3, 4):
        copies[n].start()
    tiles = CHUNK // 128
    for c in range(tiles):
        for b in range(2):
            pre[c, b, 0:8, :] = jnp.zeros((8, 128), F32)
            pre[c, b, 8 + 4 * TOK :, :] = jnp.zeros((8, 128), F32)
    keep = lax.broadcasted_iota(jnp.int32, (16, 128), 1) < SLOTS
    for n in (1, 2, 0):
        copies[n].wait()

    def expand(g, j, u):
        row = u * 16
        codes = codes_ref[j, row : row + 16, :].astype(F32)
        grad = grad_ref[j, row : row + 16, :].astype(F32)
        for side in range(2):
            if side:
                codes = pltpu.roll(codes, SLOTS, 1)
                grad = pltpu.roll(grad, SLOTS, 1)
            codes_side = jnp.where(keep, codes, 0.0)
            grad_side = jnp.where(keep, grad, 0.0)
            start = pl.multiple_of(j * TOK + side * 128 + row, 16)
            packed = inv_ref[pl.ds(start, 16), pl.ds(pl.multiple_of((g // 2) * 128, 128), 128)]
            into = pl.multiple_of(8 + (j // 2) * TOK + side * 128 + row, 8)
            for c in range(tiles):
                at = slice(c * 128, (c + 1) * 128)
                slot = slot_lane(packed, 7 * (lax.rem(g, 2) * 2 + c))
                wide = [
                    jnp.take_along_axis(codes_side[r : r + 8], slot[r : r + 8], axis=1)
                    for r in (0, 8)
                ]
                dense[pl.ds(start, 16), at] = jnp.concatenate(wide, axis=0).astype(BF16)
                for r in (0, 8):
                    pre[c, lax.rem(j, 2), pl.ds(into + r, 8), :] = jnp.take_along_axis(
                        grad_side[r : r + 8], slot[r : r + 8], axis=1
                    )

    def chunk(g, carry):
        lanes = pl.multiple_of(g * CHUNK, CHUNK)

        def expand_block(j, carry):
            for u in range(8):
                expand(g, j, u)
            return carry

        lax.fori_loop(0, GROUP, expand_block, 0)

        @pl.when(g == 0)
        def _():
            copies[3].wait()
            copies[4].wait()
            for j in range(GROUP):
                res_t[:, j * TOK : (j + 1) * TOK] = res_ref[j].T


        def spread(j, carry):
            into = pl.multiple_of(j * TOK, TOK)
            for c in range(tiles):
                taps = taps_ref[:, pl.ds(lanes + c * 128, 128)]
                for part in range(4):
                    row = (j // 2) * TOK + part * 64
                    total = jnp.zeros((64, 128), F32)
                    for k in range(TAPS):
                        total = (
                            total
                            + taps[k : k + 1]
                            * pre[c, lax.rem(j, 2), pl.ds(row + (8 + HALF - k), 64), :]
                        )
                    grad_in[pl.ds(into + part * 64, 64), c * 128 : (c + 1) * 128] = total.astype(
                        BF16
                    )
            return carry

        lax.fori_loop(0, GROUP, spread, 0)
        product[...] = jnp.dot(
            res_t[...], dense[...], preferred_element_type=F32
        ) + jnp.dot(act_t_ref[...], grad_in[...], preferred_element_type=F32)
        out_ref[:, pl.ds(lanes, CHUNK)] = product[pl.ds(pl.multiple_of(where_ref[0], 64), OWN), :]
        return carry

    lax.fori_loop(0, LATS // CHUNK, chunk, 0)


def dictionary_gradient(where, inv, codes8, grad8, res8, act_t, taps):
    return pl.pallas_call(
        dictionary_kernel,
        out_shape=jax.ShapeDtypeStruct((OWN, LATS), F32),
        in_specs=[pl.BlockSpec(memory_space=pltpu.SMEM)] + [ANY] * 5 + [VMEM],
        out_specs=VMEM,
        scratch_shapes=[
            pltpu.VMEM((GROUP * TOK, 256), jnp.int32),
            pltpu.VMEM((GROUP, 128, 128), BF16),
            pltpu.VMEM((GROUP, 128, 128), BF16),
            pltpu.VMEM((GROUP, TOK, WIN), BF16),
            pltpu.VMEM((WIN, GROUP * TOK), BF16),
            pltpu.VMEM((GROUP * TOK, CHUNK), BF16),
            pltpu.VMEM((CHUNK // 128, 2, SEQ_ROWS, 128), F32),
            pltpu.VMEM((GROUP * TOK, CHUNK), BF16),
            pltpu.VMEM((WIN, GROUP * TOK), BF16),
            pltpu.VMEM((WIN, CHUNK), F32),
            pltpu.SemaphoreType.DMA((5,)),
        ],
        compiler_params=pltpu.CompilerParams(vmem_limit_bytes=61 * 1024 * 1024),
        name="dictionary_gradient",
    )(where, inv, codes8, grad8, res8, act_t, taps)


def body(activations, dictionary, topk_ids, kernel_taps, enc_bias):
    act = activations[0]
    latents, part, dwin, lat, own_inv, ids8 = opening(
        act, dictionary, topk_ids[0].T, kernel_taps, enc_bias[None]
    )
    res8, act_t, inv = summed(part, act, ids8, own_inv)
    grad8, codes8, small = all_codes(latents, res8, dwin, ids8, own_inv, lat)
    where = (lax.axis_index("batch") * 64).astype(jnp.int32)[None]
    gradient = dictionary_gradient(where, inv, codes8, grad8, res8, act_t, kernel_taps)
    return gradient.T, small[:TAPS], small[TAPS]


def solution(mesh):
    finer = Mesh(
        mesh.devices.reshape(mesh.shape["seq"], 2, 8, 2, mesh.shape["batch"]),
        ("seq", "lat_0", "lat_1", "lat_2", "batch"),
    )
    return jax.shard_map(
        body,
        mesh=finer,
        in_specs=(
            P("batch", "seq", None),
            P(LAT, None),
            P("batch", "seq", None),
            P(None, LAT),
            P(LAT),
        ),
        out_specs=(P(LAT, ("seq", "batch")), P(None, LAT), P(LAT)),
        check_vma=False,
    )
```

```python
import functools

import jax
import jax.numpy as jnp
from jax import lax
from jax.experimental import pallas as pl
from jax.experimental.pallas import tpu as pltpu
from jax.sharding import Mesh
from jax.sharding import PartitionSpec as P

TAPS = 9
HALF = 4
LAT = ("lat_0", "lat_1", "lat_2")
D = 3584
TOK = 256
LATS = 1024
SLOTS = 64
OWN = 448
WIN = 512
GROUP = 8
PIECES = 4
F32 = jnp.float32
BF16 = jnp.bfloat16
MESH = pl.DeviceIdType.MESH
VMEM = pl.BlockSpec(memory_space=pltpu.VMEM)
ANY = pl.BlockSpec(memory_space=pl.ANY)
OPENING_MIB = 50
SUM_MIB = 52
CODES_MIB = 50
LAST_MIB = 50


def seat():
    return lax.axis_index("seq") * 2 + lax.axis_index("batch")


def peer(delta):
    j = lax.rem(seat() + delta, GROUP)
    return j, {"seq": j // 2, "batch": lax.rem(j, 2)}


def peer_from(delta):
    return lax.rem(seat() + GROUP - delta, GROUP)


def enter(partners):
    barrier = pltpu.get_barrier_semaphore()
    for device in partners:
        pl.semaphore_signal(barrier, inc=1, device_id=device, device_id_type=MESH)
    pl.semaphore_wait(barrier, len(partners))


def group_partners():
    return [peer(delta)[1] for delta in range(1, GROUP)]


def remote(src, dst, send_sem, recv_sem, device):
    return pltpu.make_async_remote_copy(
        src_ref=src,
        dst_ref=dst,
        send_sem=send_sem,
        recv_sem=recv_sem,
        device_id=device,
        device_id_type=MESH,
    )


def first_latent():
    group = lax.axis_index("lat_0") * 16 + lax.axis_index("lat_1") * 2 + lax.axis_index("lat_2")
    return group * LATS


def window(j):
    return pl.multiple_of((j * 7 // 2) * 128, 128)


def slot_rows(ids, side, first, rows_ref):
    code = ids[:, pl.ds(pl.multiple_of(side * 128, 128), 128)] - first
    inside = (code >= 0) & (code < LATS)
    hi = code >> 7
    part = hi & 3
    scale = jnp.where(
        part == 0, 1, jnp.where(part == 1, 1 << 7, jnp.where(part == 2, 1 << 14, 1 << 21))
    )
    value = (lax.broadcasted_iota(jnp.int32, (SLOTS, 128), 0) + SLOTS) * scale
    rows_ref[0] = jnp.where(inside, code & 127, -1)
    rows_ref[1] = jnp.where(inside & (hi < 4), value, 0)
    rows_ref[2] = jnp.where(inside & (hi >= 4), value, 0)


def slot_half(side, half, inv_ref, base, rows_ref, found_ref):
    sublane = lax.broadcasted_iota(jnp.int32, (8, 128), 0) + half * 64
    found = [[jnp.zeros((8, 128), jnp.int32) for _ in range(2)] for _ in range(8)]
    for k in range(SLOTS):
        low = jnp.broadcast_to(rows_ref[0, k : k + 1, :], (8, 128))
        values = [jnp.broadcast_to(rows_ref[1 + i, k : k + 1, :], (8, 128)) for i in range(2)]
        for r in range(8):
            here = low == sublane + r * 8
            for i in range(2):
                found[r][i] = found[r][i] + jnp.where(here, values[i], 0)
    for r in range(8):
        for i in range(2):
            found_ref[i, r * 8 : (r + 1) * 8, :] = found[r][i]
    into = pl.ds(pl.multiple_of(base + side * 128, 128), 128)
    for i in range(2):
        found_half = found_ref[i].T

        @pl.when(half == 0)
        def _():
            inv_ref[into, i * 128 : i * 128 + 64] = found_half

        @pl.when(half == 1)
        def _():
            inv_ref[into, i * 128 + 64 : (i + 1) * 128] = found_half


def map_slots(n, ids, inv_ref, base, first, rows_ref, found_ref):
    side, half = n // 2, lax.rem(n, 2)

    @pl.when(half == 0)
    def _():
        slot_rows(ids, side, first, rows_ref)

    slot_half(side, half, inv_ref, base, rows_ref, found_ref)


def slot_lane(packed, shift):
    return ((packed >> shift) + SLOTS) & 127


def opening_kernel(
    act_hbm, dict_ref, ids_hbm, taps_hbm, bias_hbm,
    latents_ref, part_ref, dwin_ref, lat_ref, inv_ref, ids8_ref,
    act_ref, dbuf, ids_ref, taps_ref, bias_ref, rows_ref, found_ref, dsem, id_send, id_recv, halo_send, halo_recv, own_sem,
):
    me = seat()
    seq = lax.axis_index("seq")
    ids_copy = pltpu.make_async_copy(ids_hbm, ids_ref, own_sem.at[2])
    act_copy = pltpu.make_async_copy(act_hbm, act_ref, own_sem.at[1])
    taps_copy = pltpu.make_async_copy(taps_hbm, taps_ref, own_sem.at[3])
    bias_copy = pltpu.make_async_copy(bias_hbm, bias_ref, own_sem.at[4])
    for copy in (ids_copy, act_copy):
        copy.start()
    for c in range(4):
        pltpu.make_async_copy(dict_ref.at[pl.ds(c * 256, 256)], dbuf.at[c], dsem.at[c]).start()
    for copy in (taps_copy, bias_copy):
        copy.start()
    enter(group_partners())
    ids_copy.wait()
    sends = []
    for delta in range(1, GROUP):
        _, device = peer(delta)
        copy = remote(
            ids_ref, ids8_ref.at[me], id_send.at[delta - 1], id_recv.at[delta - 1], device
        )
        copy.start()
        sends.append(copy)
    own_ids = pltpu.make_async_copy(ids_ref, ids8_ref.at[me], own_sem.at[0])
    own_ids.start()
    act_copy.wait()

    def encode(c, carry):
        pltpu.make_async_copy(dict_ref.at[pl.ds(0, 256)], dbuf.at[c], dsem.at[c]).wait()
        both = lax.dot_general(
            act_ref[...], dbuf[c], (((1,), (1,)), ((), ())), preferred_element_type=F32
        )
        lat_ref[2 * c, 8 : 8 + TOK, :] = both[:, :128]
        lat_ref[2 * c + 1, 8 : 8 + TOK, :] = both[:, 128:]
        return carry

    lax.fori_loop(0, 4, encode, 0)
    left = {"seq": lax.rem(seq + 3, 4)}
    right = {"seq": lax.rem(seq + 1, 4)}
    to_left = remote(
        lat_ref.at[:, pl.ds(8, 8)], lat_ref.at[:, pl.ds(8 + TOK, 8)],
        halo_send.at[0], halo_recv.at[0], left,
    )
    to_right = remote(
        lat_ref.at[:, pl.ds(TOK, 8)], lat_ref.at[:, pl.ds(0, 8)],
        halo_send.at[1], halo_recv.at[1], right,
    )
    to_left.start()
    to_right.start()
    dwin_ref[...] = dbuf[:, :, pl.ds(window(me), WIN)].reshape(LATS, WIN)

    def own_slots(n, carry):
        map_slots(n, ids_ref, inv_ref, 0, first_latent(), rows_ref, found_ref)
        return carry

    lax.fori_loop(0, 4, own_slots, 0)
    taps_copy.wait()
    bias_copy.wait()
    to_left.wait()
    to_right.wait()
    lat_ref[:, 0:8, :] = jnp.where(seq > 0, lat_ref[:, 0:8, :], 0.0)
    lat_ref[:, 8 + TOK :, :] = jnp.where(seq < 3, lat_ref[:, 8 + TOK :, :], 0.0)
    for c in range(8):
        at = slice(c * 128, (c + 1) * 128)
        total = jnp.zeros((TOK, 128), F32)
        for k in range(TAPS):
            total = total + taps_ref[k : k + 1, at] * lat_ref[c, k + HALF : k + HALF + TOK, :]
        total = total + bias_ref[:, at]
        packed = inv_ref[:, (c // 4) * 128 : (c // 4 + 1) * 128]
        active = ((packed >> (7 * (c % 4))) & 127) != 0
        latents_ref[:, at] = jnp.where(active, total, 0.0).astype(BF16)

    def decode(n, carry):
        at = pl.ds(pl.multiple_of(n * 512, 512), 512)
        part_ref[:, at] = jnp.dot(
            latents_ref[...], dbuf[:, :, at].reshape(LATS, 512), preferred_element_type=F32
        ).astype(BF16)
        return carry

    lax.fori_loop(0, D // 512, decode, 0)
    own_ids.wait()
    for delta in range(1, GROUP):
        pltpu.make_async_copy(ids_ref, ids8_ref.at[0], id_recv.at[delta - 1]).wait()
    for copy in sends:
        copy.wait_send()


SLOT_SCRATCH = [pltpu.VMEM((3, SLOTS, 128), jnp.int32), pltpu.VMEM((2, 64, 128), jnp.int32)]


def opening(act, dictionary, ids, taps, bias):
    return pl.pallas_call(
        opening_kernel,
        out_shape=(
            jax.ShapeDtypeStruct((TOK, LATS), BF16),
            jax.ShapeDtypeStruct((TOK, D), BF16),
            jax.ShapeDtypeStruct((LATS, WIN), BF16),
            jax.ShapeDtypeStruct((8, TOK + 16, 128), F32),
            jax.ShapeDtypeStruct((TOK, 256), jnp.int32),
            jax.ShapeDtypeStruct((GROUP, SLOTS, TOK), jnp.int32),
        ),
        in_specs=[ANY] * 5,
        out_specs=[VMEM] * 6,
        scratch_shapes=[
            pltpu.VMEM((TOK, D), BF16),
            pltpu.VMEM((4, 256, D), BF16),
            pltpu.VMEM((SLOTS, TOK), jnp.int32),
            pltpu.VMEM((TAPS, LATS), F32),
            pltpu.VMEM((1, LATS), F32),
            *SLOT_SCRATCH,
            pltpu.SemaphoreType.DMA((4,)),
            pltpu.SemaphoreType.DMA((7,)),
            pltpu.SemaphoreType.DMA((7,)),
            pltpu.SemaphoreType.DMA((2,)),
            pltpu.SemaphoreType.DMA((2,)),
            pltpu.SemaphoreType.DMA((5,)),
        ],
        compiler_params=pltpu.CompilerParams(
            collective_id=0, has_side_effects=True, vmem_limit_bytes=OPENING_MIB * 1024 * 1024
        ),
        name="opening",
    )(act, dictionary, ids, taps, bias)


def sum_kernel(
    part_hbm, act_hbm, ids8_ref, own_inv_ref, res8_ref, act_t_hbm, inv_hbm,
    part_ref, act_t_ref, inv_ref, act_ref, cols_ref, rows_ref, found_ref, half, down_out, down_in, up_out, up_in, own_sum, other_sum, res, slices,
    half_sem, dsend, drecv, usend, urecv, xsend, xrecv, asend, arecv,
    gdsend, gdrecv, gusend, gurecv, csend, crecv, act_send, act_recv, swap_send, swap_recv, own_sem,
):
    me = seat()
    core = lax.axis_index("lat_2")
    z = lax.axis_index("lat_1")
    x = lax.axis_index("lat_0")
    first = first_latent()
    other_core = {"lat_2": 1 - core}
    below = {"lat_1": lax.rem(z + 7, 8)}
    above = {"lat_1": lax.rem(z + 1, 8)}
    other_x = {"lat_0": 1 - x}
    give = pl.multiple_of((1 - core) * 128, 128)
    keep = pl.multiple_of(core * 128, 128)
    rows = pl.multiple_of(keep + z * 16, 16)

    def work(n):
        j = lax.rem(me + 1 + n // 4, GROUP)
        map_slots(
            lax.rem(n, 4), ids8_ref.at[j], inv_ref, j * TOK, first, rows_ref, found_ref
        )

    def work_many(begin, end):
        def step(n, carry):
            work(n)
            return carry

        lax.fori_loop(begin, end, step, 0)

    own_inv = pltpu.make_async_copy(
        own_inv_ref, inv_ref.at[pl.ds(pl.multiple_of(me * TOK, TOK), TOK)], own_sem.at[0]
    )
    own_inv.start()
    act_in = pltpu.make_async_copy(act_hbm, act_ref, own_sem.at[3])
    part_in = pltpu.make_async_copy(part_hbm, part_ref, own_sem.at[4])
    part_in.start()
    act_in.start()
    own_cols = pltpu.make_async_copy(
        act_ref.at[:, pl.ds(window(me), WIN)], cols_ref.at[me], own_sem.at[1]
    )
    enter([other_core, below, above, other_x] + group_partners())

    def half_copy():
        return remote(
            part_ref.at[pl.ds(give, 128)], half, half_sem.at[0], half_sem.at[1], other_core
        )

    def act_copy(delta):
        j, device = peer(delta)
        return remote(
            act_ref.at[pl.ds(keep, 128), pl.ds(window(j), WIN)],
            cols_ref.at[me, pl.ds(keep, 128)],
            act_send.at[delta - 1],
            act_recv.at[delta - 1],
            device,
        )

    def swap_copy(delta):
        rows_here = cols_ref.at[peer_from(delta), pl.ds(keep, 128)]
        return remote(
            rows_here, rows_here, swap_send.at[delta - 1], swap_recv.at[delta - 1], other_core
        )

    part_in.wait()
    half_copy().start()
    act_in.wait()
    own_cols.start()
    for delta in range(1, GROUP):
        act_copy(delta).start()
    work_many(0, 3)
    half_copy().wait_recv()
    width = D // PIECES

    def cols_of(h):
        return pl.ds(pl.multiple_of(h * width, width), width)

    def mine(chunk, h):
        at = pl.multiple_of(chunk * 16, 16)
        return part_ref[pl.ds(keep + at, 16), cols_of(h)].astype(F32) + half[
            pl.ds(at, 16), cols_of(h)
        ].astype(F32)

    def down_copy(s, h):
        return remote(
            down_out.at[s, :, cols_of(h)],
            down_in.at[s, :, cols_of(h)],
            dsend.at[s, h],
            drecv.at[s, h],
            below,
        )

    def up_copy(s, h):
        return remote(
            up_out.at[s, :, cols_of(h)],
            up_in.at[s, :, cols_of(h)],
            usend.at[s, h],
            urecv.at[s, h],
            above,
        )

    def x_copy(h):
        return remote(
            own_sum.at[:, cols_of(h)], other_sum.at[:, cols_of(h)], xsend.at[h], xrecv.at[h], other_x
        )

    def far_sums(h, carry):
        down_out[0, :, cols_of(h)] = mine(lax.rem(z + 4, 8), h).astype(BF16)
        down_copy(0, h).start()
        up_out[0, :, cols_of(h)] = mine(lax.rem(z + 3, 8), h).astype(BF16)
        up_copy(0, h).start()
        return carry

    lax.fori_loop(0, PIECES, far_sums, 0)

    def near_sums(i, carry):
        s, h = i // PIECES + 1, lax.rem(i, PIECES)
        work(3 + i)
        down_copy(s - 1, h).wait_recv()
        down_out[s, :, cols_of(h)] = (
            mine(lax.rem(z + 4 + s, 8), h) + down_in[s - 1, :, cols_of(h)].astype(F32)
        ).astype(BF16)
        down_copy(s, h).start()

        @pl.when(s <= 2)
        def _():
            up_copy(s - 1, h).wait_recv()
            up_out[s, :, cols_of(h)] = (
                mine(lax.rem(z + 3 - s, 8), h) + up_in[s - 1, :, cols_of(h)].astype(F32)
            ).astype(BF16)
            up_copy(s, h).start()

        return carry

    lax.fori_loop(0, 3 * PIECES, near_sums, 0)

    def last_sums(h, carry):
        down_copy(3, h).wait_recv()
        up_copy(2, h).wait_recv()
        total = mine(z, h) + down_in[3, :, cols_of(h)].astype(F32)
        total = total + up_in[2, :, cols_of(h)].astype(F32)
        own_sum[:, cols_of(h)] = total.astype(BF16)
        x_copy(h).start()
        return carry

    lax.fori_loop(0, PIECES, last_sums, 0)
    work_many(15, 20)
    for h in range(PIECES):
        x_copy(h).wait_recv()
    res[...] = (own_sum[...].astype(F32) + other_sum[...].astype(F32)) - act_ref[
        pl.ds(rows, 16), :
    ].astype(F32)
    for j in range(GROUP):
        begin = (j * 7 // 2) * 128
        column = lax.broadcasted_iota(jnp.int32, (16, WIN), 1) + begin
        owned = (column >= j * OWN) & (column < (j + 1) * OWN)
        slices[j] = jnp.where(owned, res[:, begin : begin + WIN], 0.0).astype(BF16)

    def slice_copy(delta):
        j, device = peer(delta)
        return remote(
            slices.at[j],
            res8_ref.at[me, pl.ds(rows, 16)],
            asend.at[delta - 1],
            arecv.at[delta - 1],
            device,
        )

    for delta in range(1, GROUP):
        slice_copy(delta).start()
    own = pltpu.make_async_copy(slices.at[me], res8_ref.at[me, pl.ds(rows, 16)], own_sem.at[2])
    own.start()
    work_many(20, 24)
    for delta in range(1, GROUP):
        act_copy(delta).wait_recv()
        swap_copy(delta).start()
    own.wait()
    for delta in range(1, GROUP):
        slice_copy(delta).wait_recv()

    def region(chunk, h):
        at = pl.multiple_of(keep + chunk * 16, 16)
        return res8_ref.at[pl.ds(h * 2, 2), pl.ds(at, 16)]

    def chunk_rows(base, chunk):
        at = pl.multiple_of(base + chunk * 16, 16)
        return res8_ref.at[:, pl.ds(at, 16)]

    def down_region(s, h):
        chunk = region(lax.rem(z + s, 8), h)
        return remote(chunk, chunk, gdsend.at[s, h], gdrecv.at[s, h], below)

    def up_region(s, h):
        chunk = region(lax.rem(z + 8 - s, 8), h)
        return remote(chunk, chunk, gusend.at[s, h], gurecv.at[s, h], above)

    def arrived(sem, chunk, h):
        pltpu.make_async_copy(region(chunk, h), region(chunk, h), sem).wait()

    def core_copy(chunk, n):
        part = chunk_rows(keep, chunk)
        return remote(part, part, csend.at[n], crecv.at[n], other_core)

    def first_regions(h, carry):
        down_region(0, h).start()
        up_region(0, h).start()
        return carry

    lax.fori_loop(0, 4, first_regions, 0)
    core_copy(z, 0).start()

    def next_regions(i, carry):
        s, h = i // 4 + 1, lax.rem(i, 4)

        @pl.when(i < 4)
        def _():
            work(24 + i)

        @pl.when(i == 4)
        def _():
            own_cols.wait()

        @pl.when(i > 4)
        def _():
            swap_copy(i - 4).wait_recv()

        @pl.when(i >= 4)
        def _():
            j = lax.rem(me + 12 - i, GROUP)
            act_t_ref[:, pl.ds(pl.multiple_of(j * TOK, TOK), TOK)] = cols_ref[j].T

        arrived(gdrecv.at[s - 1, h], lax.rem(z + s, 8), h)
        down_region(s, h).start()
        arrived(gurecv.at[s - 1, h], lax.rem(z + 8 - s, 8), h)

        @pl.when(s <= 2)
        def _():
            up_region(s, h).start()

        @pl.when(h == 3)
        def _():
            core_copy(lax.rem(z + s, 8), s).start()
            core_copy(lax.rem(z + 8 - s, 8), s + 4).start()

        return carry

    lax.fori_loop(0, 12, next_regions, 0)
    own_inv.wait()
    act_t_out = pltpu.make_async_copy(act_t_ref, act_t_hbm, own_sem.at[5])
    inv_out = pltpu.make_async_copy(inv_ref, inv_hbm, own_sem.at[6])
    act_t_out.start()
    inv_out.start()
    for h in range(4):
        arrived(gdrecv.at[3, h], lax.rem(z + 4, 8), h)
    core_copy(lax.rem(z + 4, 8), 4).start()
    for n in range(8):
        chunk = lax.rem(z + n, 8) if n < 5 else lax.rem(z + 12 - n, 8)
        part = chunk_rows(give, chunk)
        pltpu.make_async_copy(part, part, crecv.at[n]).wait()
    act_t_out.wait()
    inv_out.wait()
    for delta in range(1, GROUP):
        act_copy(delta).wait_send()
        swap_copy(delta).wait_send()
        slice_copy(delta).wait_send()
    half_copy().wait_send()
    for h in range(PIECES):
        x_copy(h).wait_send()
    for n in range(8):
        core_copy(z, n).wait_send()

    def sent(i, carry):
        s, h = i // 4, lax.rem(i, 4)
        down_copy(s, h).wait_send()
        down_region(s, h).wait_send()

        @pl.when(s <= 2)
        def _():
            up_copy(s, h).wait_send()
            up_region(s, h).wait_send()

        return carry

    lax.fori_loop(0, 16, sent, 0)


def summed(part, act, ids8, own_inv):
    dma = pltpu.SemaphoreType.DMA
    return pl.pallas_call(
        sum_kernel,
        out_shape=(
            jax.ShapeDtypeStruct((GROUP, TOK, WIN), BF16),
            jax.ShapeDtypeStruct((WIN, GROUP * TOK), BF16),
            jax.ShapeDtypeStruct((GROUP * TOK, 256), jnp.int32),
        ),
        in_specs=[ANY, ANY, VMEM, VMEM],
        out_specs=[VMEM, ANY, ANY],
        scratch_shapes=[
            pltpu.VMEM((TOK, D), BF16),
            pltpu.VMEM((WIN, GROUP * TOK), BF16),
            pltpu.VMEM((GROUP * TOK, 256), jnp.int32),
            pltpu.VMEM((TOK, D), BF16),
            pltpu.VMEM((GROUP, TOK, WIN), BF16),
            *SLOT_SCRATCH,
            pltpu.VMEM((128, D), BF16),
            pltpu.VMEM((4, 16, D), BF16),
            pltpu.VMEM((4, 16, D), BF16),
            pltpu.VMEM((3, 16, D), BF16),
            pltpu.VMEM((3, 16, D), BF16),
            pltpu.VMEM((16, D), BF16),
            pltpu.VMEM((16, D), BF16),
            pltpu.VMEM((16, D), F32),
            pltpu.VMEM((GROUP, 16, WIN), BF16),
            dma((2,)),
            dma((4, PIECES)),
            dma((4, PIECES)),
            dma((3, PIECES)),
            dma((3, PIECES)),
            dma((PIECES,)),
            dma((PIECES,)),
            dma((7,)),
            dma((7,)),
            dma((4, 4)),
            dma((4, 4)),
            dma((3, 4)),
            dma((3, 4)),
            dma((8,)),
            dma((8,)),
            dma((7,)),
            dma((7,)),
            dma((7,)),
            dma((7,)),
            dma((7,)),
        ],
        compiler_params=pltpu.CompilerParams(
            collective_id=1, has_side_effects=True, vmem_limit_bytes=SUM_MIB * 1024 * 1024
        ),
        name="summed",
    )(part, act, ids8, own_inv)


def slots_of(read, ids, first):
    def rows(row):
        local = ids[pl.ds(row, 8), :] - first
        inside = (local >= 0) & (local < LATS)
        code = jnp.where(inside, local, 8 * 128)
        low, high = code & 127, code >> 7
        second = lax.broadcasted_iota(jnp.int32, (8, 128), 1) >= SLOTS
        total = jnp.zeros((8, 128), F32)
        for c in range(8):
            one = jnp.take_along_axis(read(row, c), low, axis=1)
            two = jnp.take_along_axis(read(row + 128, c), low, axis=1)
            total = jnp.where(high == c, jnp.where(second, two, one), total)
        return total

    return rows


def pick_slots(value_ref, ids, into, first):
    def step(block, carry):
        for part in range(2):
            row = pl.multiple_of(block * 32 + part * 16, 16)
            halves = []
            for side in range(2):
                at = pl.multiple_of(row + side * 8, 8)
                rows = slots_of(
                    lambda r, c: value_ref[pl.ds(r, 8), c * 128 : (c + 1) * 128], ids, first
                )
                halves.append(rows(at))
            into[pl.ds(row, 16), :] = jnp.concatenate(halves, axis=0).astype(BF16)
        return carry

    lax.fori_loop(0, 4, step, 0)


def codes_kernel(
    latents_ref, res8_hbm, dwin, ids8_ref, inv_ref, lat_ref,
    total_ref, codes8_ref, small_ref,
    res8_ref, dense, ids_rows, codes, part, arrived, own_total, small_part, small_out, small_in,
    psend, precv, csend, crecv, tsend, trecv, ssend, srecv, own_sem,
):
    me = seat()
    first = first_latent()
    res_in = pltpu.make_async_copy(res8_hbm, res8_ref, own_sem.at[0])
    res_in.start()
    dense[...] = latents_ref[...].astype(F32)

    def rows_of(j):
        ids = ids8_ref[j]
        ids_rows[...] = jnp.concatenate([ids[:, :128], ids[:, 128:]], axis=0).T

    rows_of(me)
    pick_slots(dense, ids_rows, codes, first)
    enter(group_partners())

    def code_copy(delta):
        return remote(
            codes, codes8_ref.at[me], csend.at[delta - 1], crecv.at[delta - 1], peer(delta)[1]
        )

    def part_copy(delta):
        j, device = peer(delta)
        return remote(part.at[j], arrived.at[me], psend.at[delta - 1], precv.at[delta - 1], device)

    def total_copy(delta):
        return remote(
            own_total, total_ref.at[me], tsend.at[delta - 1], trecv.at[delta - 1], peer(delta)[1]
        )

    def small_copy(delta):
        return remote(
            small_out, small_in.at[me], ssend.at[delta - 1], srecv.at[delta - 1], peer(delta)[1]
        )

    for delta in range(1, GROUP):
        code_copy(delta).start()
    res_in.wait()

    def block(n, carry):
        j = lax.rem(me + n, GROUP)
        dense[...] = lax.dot_general(
            res8_ref[j], dwin[...], (((1,), (1,)), ((), ())), preferred_element_type=F32
        )
        rows_of(j)
        pick_slots(dense, ids_rows, part.at[j], first)

        @pl.when(n < GROUP)
        def _():
            part_copy(n).start()

        return carry

    lax.fori_loop(1, GROUP + 1, block, 0)
    for delta in range(1, GROUP):
        part_copy(delta).wait_recv()
    arrived[me] = part[me]
    total = arrived[0].astype(F32)
    for j in range(1, GROUP):
        total = total + arrived[j].astype(F32)
    own_total[...] = total.astype(BF16)
    for delta in range(1, GROUP):
        total_copy(delta).start()
    keep = lax.broadcasted_iota(jnp.int32, (8, 128), 1) < SLOTS

    def expand(step, carry):
        row = pl.multiple_of(step * 16, 16)
        both = own_total[pl.ds(row, 16), :].astype(F32)
        for side in range(2):
            values = pltpu.roll(both, SLOTS, 1) if side else both
            at = pl.multiple_of(row + side * 128, 16)
            for c in range(8):
                lanes = slice(c * 128, (c + 1) * 128)
                packed = inv_ref[pl.ds(at, 16), (c // 4) * 128 : (c // 4 + 1) * 128]
                slot = slot_lane(packed, 7 * (c % 4))
                for r in (0, 8):
                    dense[pl.ds(at + r, 8), lanes] = jnp.take_along_axis(
                        jnp.where(keep, values[r : r + 8], 0.0), slot[r : r + 8], axis=1
                    )
        return carry

    lax.fori_loop(0, 8, expand, 0)
    small_part[TAPS + 1 :, :] = jnp.zeros((16 - TAPS - 1, LATS), F32)

    def correlate(c, carry):
        lanes = pl.ds(pl.multiple_of(c * 128, 128), 128)
        own = dense[:, lanes]
        for k in range(TAPS):
            small_part[k : k + 1, lanes] = jnp.sum(
                own * lat_ref[c, k + HALF : k + HALF + TOK, :], axis=0, keepdims=True
            )
        small_part[TAPS : TAPS + 1, lanes] = jnp.sum(own, axis=0, keepdims=True)
        return carry

    lax.fori_loop(0, 8, correlate, 0)
    small_out[...] = small_part[...].astype(BF16)
    for delta in range(1, GROUP):
        small_copy(delta).start()
    own_copies = [
        pltpu.make_async_copy(own_total, total_ref.at[me], own_sem.at[1]),
        pltpu.make_async_copy(codes, codes8_ref.at[me], own_sem.at[2]),
    ]
    for copy in own_copies:
        copy.start()
    small_in[me] = small_out[...]
    for copy in own_copies:
        copy.wait()
    for delta in range(1, GROUP):
        code_copy(delta).wait_recv()
        total_copy(delta).wait_recv()
        small_copy(delta).wait_recv()
    small = small_in[0].astype(F32)
    for j in range(1, GROUP):
        small = small + small_in[j].astype(F32)
    small_ref[...] = small
    for delta in range(1, GROUP):
        code_copy(delta).wait_send()
        part_copy(delta).wait_send()
        total_copy(delta).wait_send()
        small_copy(delta).wait_send()


def all_codes(latents, res8, dwin, ids8, own_inv, lat):
    shape = jax.ShapeDtypeStruct((GROUP, 128, 128), BF16)
    dma = pltpu.SemaphoreType.DMA
    return pl.pallas_call(
        codes_kernel,
        out_shape=(shape, shape, jax.ShapeDtypeStruct((16, LATS), F32)),
        in_specs=[VMEM, ANY] + [VMEM] * 4,
        out_specs=(VMEM, VMEM, VMEM),
        scratch_shapes=[
            pltpu.VMEM((GROUP, TOK, WIN), BF16),
            pltpu.VMEM((TOK, LATS), F32),
            pltpu.VMEM((128, 128), jnp.int32),
            pltpu.VMEM((128, 128), BF16),
            pltpu.VMEM((GROUP, 128, 128), BF16),
            pltpu.VMEM((GROUP, 128, 128), BF16),
            pltpu.VMEM((128, 128), BF16),
            pltpu.VMEM((16, LATS), F32),
            pltpu.VMEM((16, LATS), BF16),
            pltpu.VMEM((GROUP, 16, LATS), BF16),
        ]
        + [dma((7,))] * 8
        + [dma((3,))],
        compiler_params=pltpu.CompilerParams(
            collective_id=2, has_side_effects=True, vmem_limit_bytes=CODES_MIB * 1024 * 1024
        ),
        name="all_codes",
    )(latents, res8, dwin, ids8, own_inv, lat)


SEQ_ROWS = 4 * TOK + 16
CHUNK = 256


def dictionary_kernel(
    where_ref, inv_hbm, res_hbm, act_t_hbm, codes_ref, grad_ref, taps_ref, small_ref,
    out_ref, taps_out_ref, bias_out_ref, inv_ref, res_ref, act_t_ref, dense, pre, grad_in, res_t, product, sems,
):
    sources = [inv_hbm, res_hbm, act_t_hbm]
    targets = [inv_ref, res_ref, act_t_ref]
    copies = [pltpu.make_async_copy(a, b, sems.at[n]) for n, (a, b) in enumerate(zip(sources, targets))]
    for copy in copies:
        copy.start()
    taps_out_ref[...] = small_ref[:TAPS, :]
    bias_out_ref[...] = small_ref[TAPS : TAPS + 1, :]
    tiles = CHUNK // 128
    for c in range(tiles):
        for b in range(2):
            pre[c, b, 0:8, :] = jnp.zeros((8, 128), F32)
            pre[c, b, 8 + 4 * TOK :, :] = jnp.zeros((8, 128), F32)
    keep = lax.broadcasted_iota(jnp.int32, (16, 128), 1) < SLOTS
    copies[0].wait()

    def expand(g, j, u):
        row = u * 16
        codes = codes_ref[j, row : row + 16, :].astype(F32)
        grad = grad_ref[j, row : row + 16, :].astype(F32)
        for side in range(2):
            if side:
                codes = pltpu.roll(codes, SLOTS, 1)
                grad = pltpu.roll(grad, SLOTS, 1)
            codes_side = jnp.where(keep, codes, 0.0)
            grad_side = jnp.where(keep, grad, 0.0)
            start = pl.multiple_of(j * TOK + side * 128 + row, 16)
            packed = inv_ref[pl.ds(start, 16), pl.ds(pl.multiple_of((g // 2) * 128, 128), 128)]
            into = pl.multiple_of(8 + (j // 2) * TOK + side * 128 + row, 8)
            for c in range(tiles):
                at = slice(c * 128, (c + 1) * 128)
                slot = slot_lane(packed, 7 * (lax.rem(g, 2) * 2 + c))
                wide = [
                    jnp.take_along_axis(codes_side[r : r + 8], slot[r : r + 8], axis=1)
                    for r in (0, 8)
                ]
                dense[pl.ds(start, 16), at] = jnp.concatenate(wide, axis=0).astype(BF16)
                for r in (0, 8):
                    pre[c, lax.rem(j, 2), pl.ds(into + r, 8), :] = jnp.take_along_axis(
                        grad_side[r : r + 8], slot[r : r + 8], axis=1
                    )

    def chunk(g, carry):
        lanes = pl.multiple_of(g * CHUNK, CHUNK)

        def expand_block(j, carry):
            for u in range(8):
                expand(g, j, u)
            return carry

        lax.fori_loop(0, GROUP, expand_block, 0)

        @pl.when(g == 0)
        def _():
            copies[1].wait()
            copies[2].wait()
            for j in range(GROUP):
                res_t[:, j * TOK : (j + 1) * TOK] = res_ref[j].T


        def spread(j, carry):
            into = pl.multiple_of(j * TOK, TOK)
            for c in range(tiles):
                taps = taps_ref[:, pl.ds(lanes + c * 128, 128)]
                for part in range(4):
                    row = (j // 2) * TOK + part * 64
                    total = jnp.zeros((64, 128), F32)
                    for k in range(TAPS):
                        total = (
                            total
                            + taps[k : k + 1]
                            * pre[c, lax.rem(j, 2), pl.ds(row + (8 + HALF - k), 64), :]
                        )
                    grad_in[pl.ds(into + part * 64, 64), c * 128 : (c + 1) * 128] = total.astype(
                        BF16
                    )
            return carry

        lax.fori_loop(0, GROUP, spread, 0)
        product[...] = jnp.dot(
            res_t[...], dense[...], preferred_element_type=F32
        ) + jnp.dot(act_t_ref[...], grad_in[...], preferred_element_type=F32)
        out_ref[:, pl.ds(lanes, CHUNK)] = product[pl.ds(pl.multiple_of(where_ref[0], 64), OWN), :]
        return carry

    lax.fori_loop(0, LATS // CHUNK, chunk, 0)


def dictionary_gradient(where, inv, res8, act_t, codes8, grad8, taps, small):
    return pl.pallas_call(
        dictionary_kernel,
        out_shape=(
            jax.ShapeDtypeStruct((OWN, LATS), F32),
            jax.ShapeDtypeStruct((TAPS, LATS), F32),
            jax.ShapeDtypeStruct((1, LATS), F32),
        ),
        in_specs=[pl.BlockSpec(memory_space=pltpu.SMEM)] + [ANY] * 3 + [VMEM] * 4,
        out_specs=(VMEM, VMEM, VMEM),
        scratch_shapes=[
            pltpu.VMEM((GROUP * TOK, 256), jnp.int32),
            pltpu.VMEM((GROUP, TOK, WIN), BF16),
            pltpu.VMEM((WIN, GROUP * TOK), BF16),
            pltpu.VMEM((GROUP * TOK, CHUNK), BF16),
            pltpu.VMEM((CHUNK // 128, 2, SEQ_ROWS, 128), F32),
            pltpu.VMEM((GROUP * TOK, CHUNK), BF16),
            pltpu.VMEM((WIN, GROUP * TOK), BF16),
            pltpu.VMEM((WIN, CHUNK), F32),
            pltpu.SemaphoreType.DMA((3,)),
        ],
        compiler_params=pltpu.CompilerParams(vmem_limit_bytes=LAST_MIB * 1024 * 1024),
        name="dictionary_gradient",
    )(where, inv, res8, act_t, codes8, grad8, taps, small)


def body(activations, dictionary, topk_ids, kernel_taps, enc_bias):
    act = activations[0]
    latents, part, dwin, lat, own_inv, ids8 = opening(
        act, dictionary, topk_ids[0].T, kernel_taps, enc_bias[None]
    )
    res8, act_t, inv = summed(part, act, ids8, own_inv)
    grad8, codes8, small = all_codes(latents, res8, dwin, ids8, own_inv, lat)
    where = (lax.axis_index("batch") * 64).astype(jnp.int32)[None]
    gradient, grad_taps, grad_bias = dictionary_gradient(
        where, inv, res8, act_t, codes8, grad8, kernel_taps, small
    )
    return gradient.T, grad_taps, grad_bias[0]


def solution(mesh):
    finer = Mesh(
        mesh.devices.reshape(mesh.shape["seq"], 2, 8, 2, mesh.shape["batch"]),
        ("seq", "lat_0", "lat_1", "lat_2", "batch"),
    )
    return jax.shard_map(
        body,
        mesh=finer,
        in_specs=(
            P("batch", "seq", None),
            P(LAT, None),
            P("batch", "seq", None),
            P(None, LAT),
            P(LAT),
        ),
        out_specs=(P(LAT, ("seq", "batch")), P(None, LAT), P(LAT)),
        check_vma=False,
    )
```

```python
import functools

import jax
import jax.numpy as jnp
from jax import lax
from jax.experimental import pallas as pl
from jax.experimental.pallas import tpu as pltpu
from jax.sharding import Mesh
from jax.sharding import PartitionSpec as P

TAPS = 9
HALF = 4
LAT = ("lat_0", "lat_1", "lat_2")
D = 3584
TOK = 256
LATS = 1024
SLOTS = 64
OWN = 448
WIN = 512
GROUP = 8
PIECES = 4
F32 = jnp.float32
BF16 = jnp.bfloat16
MESH = pl.DeviceIdType.MESH
VMEM = pl.BlockSpec(memory_space=pltpu.VMEM)
ANY = pl.BlockSpec(memory_space=pl.ANY)
OPENING_MIB = 50
SUM_MIB = 52
CODES_MIB = 50
LAST_MIB = 50


def seat():
    return lax.axis_index("seq") * 2 + lax.axis_index("batch")


def peer(delta):
    j = lax.rem(seat() + delta, GROUP)
    return j, {"seq": j // 2, "batch": lax.rem(j, 2)}


def peer_from(delta):
    return lax.rem(seat() + GROUP - delta, GROUP)


def enter(partners):
    barrier = pltpu.get_barrier_semaphore()
    for device in partners:
        pl.semaphore_signal(barrier, inc=1, device_id=device, device_id_type=MESH)
    pl.semaphore_wait(barrier, len(partners))


def group_partners():
    return [peer(delta)[1] for delta in range(1, GROUP)]


def remote(src, dst, send_sem, recv_sem, device):
    return pltpu.make_async_remote_copy(
        src_ref=src,
        dst_ref=dst,
        send_sem=send_sem,
        recv_sem=recv_sem,
        device_id=device,
        device_id_type=MESH,
    )


def first_latent():
    group = lax.axis_index("lat_0") * 16 + lax.axis_index("lat_1") * 2 + lax.axis_index("lat_2")
    return group * LATS


def window(j):
    return pl.multiple_of((j * 7 // 2) * 128, 128)


def slot_rows(ids, side, first, rows_ref):
    code = ids[:, pl.ds(pl.multiple_of(side * 128, 128), 128)] - first
    inside = (code >= 0) & (code < LATS)
    hi = code >> 7
    part = hi & 3
    scale = jnp.where(
        part == 0, 1, jnp.where(part == 1, 1 << 7, jnp.where(part == 2, 1 << 14, 1 << 21))
    )
    value = (lax.broadcasted_iota(jnp.int32, (SLOTS, 128), 0) + SLOTS) * scale
    rows_ref[0] = jnp.where(inside, code & 127, -1)
    rows_ref[1] = jnp.where(inside & (hi < 4), value, 0)
    rows_ref[2] = jnp.where(inside & (hi >= 4), value, 0)


def slot_half(side, half, inv_ref, base, rows_ref, found_ref):
    sublane = lax.broadcasted_iota(jnp.int32, (8, 128), 0) + half * 64
    found = [[jnp.zeros((8, 128), jnp.int32) for _ in range(2)] for _ in range(8)]
    for k in range(SLOTS):
        low = jnp.broadcast_to(rows_ref[0, k : k + 1, :], (8, 128))
        values = [jnp.broadcast_to(rows_ref[1 + i, k : k + 1, :], (8, 128)) for i in range(2)]
        for r in range(8):
            here = low == sublane + r * 8
            for i in range(2):
                found[r][i] = found[r][i] + jnp.where(here, values[i], 0)
    for r in range(8):
        for i in range(2):
            found_ref[i, r * 8 : (r + 1) * 8, :] = found[r][i]
    into = pl.ds(pl.multiple_of(base + side * 128, 128), 128)
    for i in range(2):
        found_half = found_ref[i].T

        @pl.when(half == 0)
        def _():
            inv_ref[into, i * 128 : i * 128 + 64] = found_half

        @pl.when(half == 1)
        def _():
            inv_ref[into, i * 128 + 64 : (i + 1) * 128] = found_half


def map_slots(n, ids, inv_ref, base, first, rows_ref, found_ref):
    side, half = n // 2, lax.rem(n, 2)

    @pl.when(half == 0)
    def _():
        slot_rows(ids, side, first, rows_ref)

    slot_half(side, half, inv_ref, base, rows_ref, found_ref)


def slot_lane(packed, shift):
    return ((packed >> shift) + SLOTS) & 127


def opening_kernel(
    act_hbm, dict_ref, ids_hbm, taps_hbm, bias_hbm,
    latents_ref, part_ref, dwin_ref, lat_ref, inv_ref, ids8_ref,
    act_ref, dbuf, ids_ref, taps_ref, bias_ref, rows_ref, found_ref, dsem, id_send, id_recv, halo_send, halo_recv, own_sem,
):
    me = seat()
    seq = lax.axis_index("seq")
    ids_copy = pltpu.make_async_copy(ids_hbm, ids_ref, own_sem.at[2])
    act_copy = pltpu.make_async_copy(act_hbm, act_ref, own_sem.at[1])
    taps_copy = pltpu.make_async_copy(taps_hbm, taps_ref, own_sem.at[3])
    bias_copy = pltpu.make_async_copy(bias_hbm, bias_ref, own_sem.at[4])
    for copy in (ids_copy, act_copy):
        copy.start()
    for c in range(4):
        pltpu.make_async_copy(dict_ref.at[pl.ds(c * 256, 256)], dbuf.at[c], dsem.at[c]).start()
    for copy in (taps_copy, bias_copy):
        copy.start()
    enter(group_partners())
    ids_copy.wait()
    sends = []
    for delta in range(1, GROUP):
        _, device = peer(delta)
        copy = remote(
            ids_ref, ids8_ref.at[me], id_send.at[delta - 1], id_recv.at[delta - 1], device
        )
        copy.start()
        sends.append(copy)
    own_ids = pltpu.make_async_copy(ids_ref, ids8_ref.at[me], own_sem.at[0])
    own_ids.start()
    act_copy.wait()

    def encode(c, carry):
        pltpu.make_async_copy(dict_ref.at[pl.ds(0, 256)], dbuf.at[c], dsem.at[c]).wait()
        both = lax.dot_general(
            act_ref[...], dbuf[c], (((1,), (1,)), ((), ())), preferred_element_type=F32
        )
        lat_ref[2 * c, 8 : 8 + TOK, :] = both[:, :128]
        lat_ref[2 * c + 1, 8 : 8 + TOK, :] = both[:, 128:]
        return carry

    lax.fori_loop(0, 4, encode, 0)
    left = {"seq": lax.rem(seq + 3, 4)}
    right = {"seq": lax.rem(seq + 1, 4)}
    to_left = remote(
        lat_ref.at[:, pl.ds(8, 8)], lat_ref.at[:, pl.ds(8 + TOK, 8)],
        halo_send.at[0], halo_recv.at[0], left,
    )
    to_right = remote(
        lat_ref.at[:, pl.ds(TOK, 8)], lat_ref.at[:, pl.ds(0, 8)],
        halo_send.at[1], halo_recv.at[1], right,
    )
    to_left.start()
    to_right.start()
    dwin_ref[...] = dbuf[:, :, pl.ds(window(me), WIN)].reshape(LATS, WIN)

    def own_slots(n, carry):
        map_slots(n, ids_ref, inv_ref, 0, first_latent(), rows_ref, found_ref)
        return carry

    lax.fori_loop(0, 4, own_slots, 0)
    taps_copy.wait()
    bias_copy.wait()
    to_left.wait()
    to_right.wait()
    lat_ref[:, 0:8, :] = jnp.where(seq > 0, lat_ref[:, 0:8, :], 0.0)
    lat_ref[:, 8 + TOK :, :] = jnp.where(seq < 3, lat_ref[:, 8 + TOK :, :], 0.0)
    for c in range(8):
        at = slice(c * 128, (c + 1) * 128)
        total = jnp.zeros((TOK, 128), F32)
        for k in range(TAPS):
            total = total + taps_ref[k : k + 1, at] * lat_ref[c, k + HALF : k + HALF + TOK, :]
        total = total + bias_ref[:, at]
        packed = inv_ref[:, (c // 4) * 128 : (c // 4 + 1) * 128]
        active = ((packed >> (7 * (c % 4))) & 127) != 0
        latents_ref[:, at] = jnp.where(active, total, 0.0).astype(BF16)

    def decode(n, carry):
        at = pl.ds(pl.multiple_of(n * 512, 512), 512)
        part_ref[:, at] = jnp.dot(
            latents_ref[...], dbuf[:, :, at].reshape(LATS, 512), preferred_element_type=F32
        ).astype(BF16)
        return carry

    lax.fori_loop(0, D // 512, decode, 0)
    own_ids.wait()
    for delta in range(1, GROUP):
        pltpu.make_async_copy(ids_ref, ids8_ref.at[0], id_recv.at[delta - 1]).wait()
    for copy in sends:
        copy.wait_send()


SLOT_SCRATCH = [pltpu.VMEM((3, SLOTS, 128), jnp.int32), pltpu.VMEM((2, 64, 128), jnp.int32)]


def opening(act, dictionary, ids, taps, bias):
    return pl.pallas_call(
        opening_kernel,
        out_shape=(
            jax.ShapeDtypeStruct((TOK, LATS), BF16),
            jax.ShapeDtypeStruct((TOK, D), BF16),
            jax.ShapeDtypeStruct((LATS, WIN), BF16),
            jax.ShapeDtypeStruct((8, TOK + 16, 128), F32),
            jax.ShapeDtypeStruct((TOK, 256), jnp.int32),
            jax.ShapeDtypeStruct((GROUP, SLOTS, TOK), jnp.int32),
        ),
        in_specs=[ANY] * 5,
        out_specs=[VMEM] * 6,
        scratch_shapes=[
            pltpu.VMEM((TOK, D), BF16),
            pltpu.VMEM((4, 256, D), BF16),
            pltpu.VMEM((SLOTS, TOK), jnp.int32),
            pltpu.VMEM((TAPS, LATS), F32),
            pltpu.VMEM((1, LATS), F32),
            *SLOT_SCRATCH,
            pltpu.SemaphoreType.DMA((4,)),
            pltpu.SemaphoreType.DMA((7,)),
            pltpu.SemaphoreType.DMA((7,)),
            pltpu.SemaphoreType.DMA((2,)),
            pltpu.SemaphoreType.DMA((2,)),
            pltpu.SemaphoreType.DMA((5,)),
        ],
        compiler_params=pltpu.CompilerParams(
            collective_id=0, has_side_effects=True, vmem_limit_bytes=OPENING_MIB * 1024 * 1024
        ),
        name="opening",
    )(act, dictionary, ids, taps, bias)


def sum_kernel(
    part_hbm, act_hbm, ids8_ref, own_inv_ref, res8_ref, act_t_hbm, inv_hbm,
    part_ref, act_t_ref, inv_ref, act_ref, cols_ref, rows_ref, found_ref, half, down_out, down_in, up_out, up_in, own_sum, other_sum, res, slices,
    half_sem, dsend, drecv, usend, urecv, xsend, xrecv, asend, arecv,
    gdsend, gdrecv, gusend, gurecv, csend, crecv, act_send, act_recv, swap_send, swap_recv, own_sem,
):
    me = seat()
    core = lax.axis_index("lat_2")
    z = lax.axis_index("lat_1")
    x = lax.axis_index("lat_0")
    first = first_latent()
    other_core = {"lat_2": 1 - core}
    below = {"lat_1": lax.rem(z + 7, 8)}
    above = {"lat_1": lax.rem(z + 1, 8)}
    other_x = {"lat_0": 1 - x}
    give = pl.multiple_of((1 - core) * 128, 128)
    keep = pl.multiple_of(core * 128, 128)
    rows = pl.multiple_of(keep + z * 16, 16)

    def work(n):
        j = lax.rem(me + 1 + n // 4, GROUP)
        map_slots(
            lax.rem(n, 4), ids8_ref.at[j], inv_ref, j * TOK, first, rows_ref, found_ref
        )

    def work_many(begin, end):
        def step(n, carry):
            work(n)
            return carry

        lax.fori_loop(begin, end, step, 0)

    own_inv = pltpu.make_async_copy(
        own_inv_ref, inv_ref.at[pl.ds(pl.multiple_of(me * TOK, TOK), TOK)], own_sem.at[0]
    )
    own_inv.start()
    act_in = pltpu.make_async_copy(act_hbm, act_ref, own_sem.at[3])
    part_in = pltpu.make_async_copy(part_hbm, part_ref, own_sem.at[4])
    part_in.start()
    act_in.start()
    own_cols = pltpu.make_async_copy(
        act_ref.at[:, pl.ds(window(me), WIN)], cols_ref.at[me], own_sem.at[1]
    )
    partners = [other_core, below, above, other_x] + group_partners()
    barrier = pltpu.get_barrier_semaphore()
    for device in partners:
        pl.semaphore_signal(barrier, inc=1, device_id=device, device_id_type=MESH)
    work_many(0, 4)
    pl.semaphore_wait(barrier, len(partners))

    def half_copy():
        return remote(
            part_ref.at[pl.ds(give, 128)], half, half_sem.at[0], half_sem.at[1], other_core
        )

    def act_copy(delta):
        j, device = peer(delta)
        return remote(
            act_ref.at[pl.ds(keep, 128), pl.ds(window(j), WIN)],
            cols_ref.at[me, pl.ds(keep, 128)],
            act_send.at[delta - 1],
            act_recv.at[delta - 1],
            device,
        )

    def swap_copy(delta):
        rows_here = cols_ref.at[peer_from(delta), pl.ds(keep, 128)]
        return remote(
            rows_here, rows_here, swap_send.at[delta - 1], swap_recv.at[delta - 1], other_core
        )

    part_in.wait()
    half_copy().start()
    act_in.wait()
    own_cols.start()
    for delta in range(1, GROUP):
        act_copy(delta).start()
    work_many(4, 7)
    half_copy().wait_recv()
    width = D // PIECES

    def cols_of(h):
        return pl.ds(pl.multiple_of(h * width, width), width)

    def mine(chunk, h):
        at = pl.multiple_of(chunk * 16, 16)
        return part_ref[pl.ds(keep + at, 16), cols_of(h)].astype(F32) + half[
            pl.ds(at, 16), cols_of(h)
        ].astype(F32)

    def down_copy(s, h):
        return remote(
            down_out.at[s, :, cols_of(h)],
            down_in.at[s, :, cols_of(h)],
            dsend.at[s, h],
            drecv.at[s, h],
            below,
        )

    def up_copy(s, h):
        return remote(
            up_out.at[s, :, cols_of(h)],
            up_in.at[s, :, cols_of(h)],
            usend.at[s, h],
            urecv.at[s, h],
            above,
        )

    def x_copy(h):
        return remote(
            own_sum.at[:, cols_of(h)], other_sum.at[:, cols_of(h)], xsend.at[h], xrecv.at[h], other_x
        )

    def far_sums(h, carry):
        down_out[0, :, cols_of(h)] = mine(lax.rem(z + 4, 8), h).astype(BF16)
        down_copy(0, h).start()
        up_out[0, :, cols_of(h)] = mine(lax.rem(z + 3, 8), h).astype(BF16)
        up_copy(0, h).start()
        return carry

    lax.fori_loop(0, PIECES, far_sums, 0)

    def near_sums(i, carry):
        s, h = i // PIECES + 1, lax.rem(i, PIECES)
        work(7 + i)
        down_copy(s - 1, h).wait_recv()
        down_out[s, :, cols_of(h)] = (
            mine(lax.rem(z + 4 + s, 8), h) + down_in[s - 1, :, cols_of(h)].astype(F32)
        ).astype(BF16)
        down_copy(s, h).start()

        @pl.when(s <= 2)
        def _():
            up_copy(s - 1, h).wait_recv()
            up_out[s, :, cols_of(h)] = (
                mine(lax.rem(z + 3 - s, 8), h) + up_in[s - 1, :, cols_of(h)].astype(F32)
            ).astype(BF16)
            up_copy(s, h).start()

        return carry

    lax.fori_loop(0, 3 * PIECES, near_sums, 0)

    def last_sums(h, carry):
        down_copy(3, h).wait_recv()
        up_copy(2, h).wait_recv()
        total = mine(z, h) + down_in[3, :, cols_of(h)].astype(F32)
        total = total + up_in[2, :, cols_of(h)].astype(F32)
        own_sum[:, cols_of(h)] = total.astype(BF16)
        x_copy(h).start()
        return carry

    lax.fori_loop(0, PIECES, last_sums, 0)
    work_many(19, 24)
    for h in range(PIECES):
        x_copy(h).wait_recv()
    res[...] = (own_sum[...].astype(F32) + other_sum[...].astype(F32)) - act_ref[
        pl.ds(rows, 16), :
    ].astype(F32)
    for j in range(GROUP):
        begin = (j * 7 // 2) * 128
        column = lax.broadcasted_iota(jnp.int32, (16, WIN), 1) + begin
        owned = (column >= j * OWN) & (column < (j + 1) * OWN)
        slices[j] = jnp.where(owned, res[:, begin : begin + WIN], 0.0).astype(BF16)

    def slice_copy(delta):
        j, device = peer(delta)
        return remote(
            slices.at[j],
            res8_ref.at[me, pl.ds(rows, 16)],
            asend.at[delta - 1],
            arecv.at[delta - 1],
            device,
        )

    for delta in range(1, GROUP):
        slice_copy(delta).start()
    own = pltpu.make_async_copy(slices.at[me], res8_ref.at[me, pl.ds(rows, 16)], own_sem.at[2])
    own.start()
    work_many(24, 28)
    for delta in range(1, GROUP):
        act_copy(delta).wait_recv()
        swap_copy(delta).start()
    own.wait()
    for delta in range(1, GROUP):
        slice_copy(delta).wait_recv()

    def region(chunk, h):
        at = pl.multiple_of(keep + chunk * 16, 16)
        return res8_ref.at[pl.ds(h * 2, 2), pl.ds(at, 16)]

    def chunk_rows(base, chunk):
        at = pl.multiple_of(base + chunk * 16, 16)
        return res8_ref.at[:, pl.ds(at, 16)]

    def down_region(s, h):
        chunk = region(lax.rem(z + s, 8), h)
        return remote(chunk, chunk, gdsend.at[s, h], gdrecv.at[s, h], below)

    def up_region(s, h):
        chunk = region(lax.rem(z + 8 - s, 8), h)
        return remote(chunk, chunk, gusend.at[s, h], gurecv.at[s, h], above)

    def arrived(sem, chunk, h):
        pltpu.make_async_copy(region(chunk, h), region(chunk, h), sem).wait()

    def core_copy(chunk, n):
        part = chunk_rows(keep, chunk)
        return remote(part, part, csend.at[n], crecv.at[n], other_core)

    def first_regions(h, carry):
        down_region(0, h).start()
        up_region(0, h).start()
        return carry

    lax.fori_loop(0, 4, first_regions, 0)
    core_copy(z, 0).start()

    def next_regions(i, carry):
        s, h = i // 4 + 1, lax.rem(i, 4)

        @pl.when(i == 4)
        def _():
            own_cols.wait()

        @pl.when(i > 4)
        def _():
            swap_copy(i - 4).wait_recv()

        @pl.when(i >= 4)
        def _():
            j = lax.rem(me + 12 - i, GROUP)
            act_t_ref[:, pl.ds(pl.multiple_of(j * TOK, TOK), TOK)] = cols_ref[j].T

        arrived(gdrecv.at[s - 1, h], lax.rem(z + s, 8), h)
        down_region(s, h).start()
        arrived(gurecv.at[s - 1, h], lax.rem(z + 8 - s, 8), h)

        @pl.when(s <= 2)
        def _():
            up_region(s, h).start()

        @pl.when(h == 3)
        def _():
            core_copy(lax.rem(z + s, 8), s).start()
            core_copy(lax.rem(z + 8 - s, 8), s + 4).start()

        return carry

    lax.fori_loop(0, 12, next_regions, 0)
    own_inv.wait()
    act_t_out = pltpu.make_async_copy(act_t_ref, act_t_hbm, own_sem.at[5])
    inv_out = pltpu.make_async_copy(inv_ref, inv_hbm, own_sem.at[6])
    act_t_out.start()
    inv_out.start()
    for h in range(4):
        arrived(gdrecv.at[3, h], lax.rem(z + 4, 8), h)
    core_copy(lax.rem(z + 4, 8), 4).start()
    for n in range(8):
        chunk = lax.rem(z + n, 8) if n < 5 else lax.rem(z + 12 - n, 8)
        part = chunk_rows(give, chunk)
        pltpu.make_async_copy(part, part, crecv.at[n]).wait()
    act_t_out.wait()
    inv_out.wait()
    for delta in range(1, GROUP):
        act_copy(delta).wait_send()
        swap_copy(delta).wait_send()
        slice_copy(delta).wait_send()
    half_copy().wait_send()
    for h in range(PIECES):
        x_copy(h).wait_send()
    for n in range(8):
        core_copy(z, n).wait_send()

    def sent(i, carry):
        s, h = i // 4, lax.rem(i, 4)
        down_copy(s, h).wait_send()
        down_region(s, h).wait_send()

        @pl.when(s <= 2)
        def _():
            up_copy(s, h).wait_send()
            up_region(s, h).wait_send()

        return carry

    lax.fori_loop(0, 16, sent, 0)


def summed(part, act, ids8, own_inv):
    dma = pltpu.SemaphoreType.DMA
    return pl.pallas_call(
        sum_kernel,
        out_shape=(
            jax.ShapeDtypeStruct((GROUP, TOK, WIN), BF16),
            jax.ShapeDtypeStruct((WIN, GROUP * TOK), BF16),
            jax.ShapeDtypeStruct((GROUP * TOK, 256), jnp.int32),
        ),
        in_specs=[ANY, ANY, VMEM, VMEM],
        out_specs=[VMEM, ANY, ANY],
        scratch_shapes=[
            pltpu.VMEM((TOK, D), BF16),
            pltpu.VMEM((WIN, GROUP * TOK), BF16),
            pltpu.VMEM((GROUP * TOK, 256), jnp.int32),
            pltpu.VMEM((TOK, D), BF16),
            pltpu.VMEM((GROUP, TOK, WIN), BF16),
            *SLOT_SCRATCH,
            pltpu.VMEM((128, D), BF16),
            pltpu.VMEM((4, 16, D), BF16),
            pltpu.VMEM((4, 16, D), BF16),
            pltpu.VMEM((3, 16, D), BF16),
            pltpu.VMEM((3, 16, D), BF16),
            pltpu.VMEM((16, D), BF16),
            pltpu.VMEM((16, D), BF16),
            pltpu.VMEM((16, D), F32),
            pltpu.VMEM((GROUP, 16, WIN), BF16),
            dma((2,)),
            dma((4, PIECES)),
            dma((4, PIECES)),
            dma((3, PIECES)),
            dma((3, PIECES)),
            dma((PIECES,)),
            dma((PIECES,)),
            dma((7,)),
            dma((7,)),
            dma((4, 4)),
            dma((4, 4)),
            dma((3, 4)),
            dma((3, 4)),
            dma((8,)),
            dma((8,)),
            dma((7,)),
            dma((7,)),
            dma((7,)),
            dma((7,)),
            dma((7,)),
        ],
        compiler_params=pltpu.CompilerParams(
            collective_id=1, has_side_effects=True, vmem_limit_bytes=SUM_MIB * 1024 * 1024
        ),
        name="summed",
    )(part, act, ids8, own_inv)


def slots_of(read, ids, first):
    def rows(row):
        local = ids[pl.ds(row, 8), :] - first
        inside = (local >= 0) & (local < LATS)
        code = jnp.where(inside, local, 8 * 128)
        low, high = code & 127, code >> 7
        second = lax.broadcasted_iota(jnp.int32, (8, 128), 1) >= SLOTS
        total = jnp.zeros((8, 128), F32)
        for c in range(8):
            one = jnp.take_along_axis(read(row, c), low, axis=1)
            two = jnp.take_along_axis(read(row + 128, c), low, axis=1)
            total = jnp.where(high == c, jnp.where(second, two, one), total)
        return total

    return rows


def pick_slots(value_ref, ids, into, first):
    def step(block, carry):
        for part in range(2):
            row = pl.multiple_of(block * 32 + part * 16, 16)
            halves = []
            for side in range(2):
                at = pl.multiple_of(row + side * 8, 8)
                rows = slots_of(
                    lambda r, c: value_ref[pl.ds(r, 8), c * 128 : (c + 1) * 128], ids, first
                )
                halves.append(rows(at))
            into[pl.ds(row, 16), :] = jnp.concatenate(halves, axis=0).astype(BF16)
        return carry

    lax.fori_loop(0, 4, step, 0)


def codes_kernel(
    latents_ref, res8_hbm, dwin, ids8_ref, inv_ref, lat_ref,
    total_ref, codes8_ref, small_ref,
    res8_ref, dense, ids_rows, codes, part, arrived, own_total, small_part, small_out, small_in,
    psend, precv, csend, crecv, tsend, trecv, ssend, srecv, own_sem,
):
    me = seat()
    first = first_latent()
    res_in = pltpu.make_async_copy(res8_hbm, res8_ref, own_sem.at[0])
    res_in.start()
    dense[...] = latents_ref[...].astype(F32)

    def rows_of(j):
        ids = ids8_ref[j]
        ids_rows[...] = jnp.concatenate([ids[:, :128], ids[:, 128:]], axis=0).T

    rows_of(me)
    pick_slots(dense, ids_rows, codes, first)
    enter(group_partners())

    def code_copy(delta):
        return remote(
            codes, codes8_ref.at[me], csend.at[delta - 1], crecv.at[delta - 1], peer(delta)[1]
        )

    def part_copy(delta):
        j, device = peer(delta)
        return remote(part.at[j], arrived.at[me], psend.at[delta - 1], precv.at[delta - 1], device)

    def total_copy(delta):
        return remote(
            own_total, total_ref.at[me], tsend.at[delta - 1], trecv.at[delta - 1], peer(delta)[1]
        )

    def small_copy(delta):
        return remote(
            small_out, small_in.at[me], ssend.at[delta - 1], srecv.at[delta - 1], peer(delta)[1]
        )

    for delta in range(1, GROUP):
        code_copy(delta).start()
    res_in.wait()

    def block(n, carry):
        j = lax.rem(me + n, GROUP)
        dense[...] = lax.dot_general(
            res8_ref[j], dwin[...], (((1,), (1,)), ((), ())), preferred_element_type=F32
        )
        rows_of(j)
        pick_slots(dense, ids_rows, part.at[j], first)

        @pl.when(n < GROUP)
        def _():
            part_copy(n).start()

        return carry

    lax.fori_loop(1, GROUP + 1, block, 0)
    for delta in range(1, GROUP):
        part_copy(delta).wait_recv()
    arrived[me] = part[me]
    total = arrived[0].astype(F32)
    for j in range(1, GROUP):
        total = total + arrived[j].astype(F32)
    own_total[...] = total.astype(BF16)
    for delta in range(1, GROUP):
        total_copy(delta).start()
    keep = lax.broadcasted_iota(jnp.int32, (8, 128), 1) < SLOTS

    def expand(step, carry):
        row = pl.multiple_of(step * 16, 16)
        both = own_total[pl.ds(row, 16), :].astype(F32)
        for side in range(2):
            values = pltpu.roll(both, SLOTS, 1) if side else both
            at = pl.multiple_of(row + side * 128, 16)
            for c in range(8):
                lanes = slice(c * 128, (c + 1) * 128)
                packed = inv_ref[pl.ds(at, 16), (c // 4) * 128 : (c // 4 + 1) * 128]
                slot = slot_lane(packed, 7 * (c % 4))
                for r in (0, 8):
                    dense[pl.ds(at + r, 8), lanes] = jnp.take_along_axis(
                        jnp.where(keep, values[r : r + 8], 0.0), slot[r : r + 8], axis=1
                    )
        return carry

    lax.fori_loop(0, 8, expand, 0)
    small_part[TAPS + 1 :, :] = jnp.zeros((16 - TAPS - 1, LATS), F32)

    def correlate(c, carry):
        lanes = pl.ds(pl.multiple_of(c * 128, 128), 128)
        own = dense[:, lanes]
        for k in range(TAPS):
            small_part[k : k + 1, lanes] = jnp.sum(
                own * lat_ref[c, k + HALF : k + HALF + TOK, :], axis=0, keepdims=True
            )
        small_part[TAPS : TAPS + 1, lanes] = jnp.sum(own, axis=0, keepdims=True)
        return carry

    lax.fori_loop(0, 8, correlate, 0)
    small_out[...] = small_part[...].astype(BF16)
    for delta in range(1, GROUP):
        small_copy(delta).start()
    own_copies = [
        pltpu.make_async_copy(own_total, total_ref.at[me], own_sem.at[1]),
        pltpu.make_async_copy(codes, codes8_ref.at[me], own_sem.at[2]),
    ]
    for copy in own_copies:
        copy.start()
    small_in[me] = small_out[...]
    for copy in own_copies:
        copy.wait()
    for delta in range(1, GROUP):
        code_copy(delta).wait_recv()
        total_copy(delta).wait_recv()
        small_copy(delta).wait_recv()
    small = small_in[0].astype(F32)
    for j in range(1, GROUP):
        small = small + small_in[j].astype(F32)
    small_ref[...] = small
    for delta in range(1, GROUP):
        code_copy(delta).wait_send()
        part_copy(delta).wait_send()
        total_copy(delta).wait_send()
        small_copy(delta).wait_send()


def all_codes(latents, res8, dwin, ids8, own_inv, lat):
    shape = jax.ShapeDtypeStruct((GROUP, 128, 128), BF16)
    dma = pltpu.SemaphoreType.DMA
    return pl.pallas_call(
        codes_kernel,
        out_shape=(shape, shape, jax.ShapeDtypeStruct((16, LATS), F32)),
        in_specs=[VMEM, ANY] + [VMEM] * 4,
        out_specs=(VMEM, VMEM, VMEM),
        scratch_shapes=[
            pltpu.VMEM((GROUP, TOK, WIN), BF16),
            pltpu.VMEM((TOK, LATS), F32),
            pltpu.VMEM((128, 128), jnp.int32),
            pltpu.VMEM((128, 128), BF16),
            pltpu.VMEM((GROUP, 128, 128), BF16),
            pltpu.VMEM((GROUP, 128, 128), BF16),
            pltpu.VMEM((128, 128), BF16),
            pltpu.VMEM((16, LATS), F32),
            pltpu.VMEM((16, LATS), BF16),
            pltpu.VMEM((GROUP, 16, LATS), BF16),
        ]
        + [dma((7,))] * 8
        + [dma((3,))],
        compiler_params=pltpu.CompilerParams(
            collective_id=2, has_side_effects=True, vmem_limit_bytes=CODES_MIB * 1024 * 1024
        ),
        name="all_codes",
    )(latents, res8, dwin, ids8, own_inv, lat)


SEQ_ROWS = 4 * TOK + 16
CHUNK = 256


def dictionary_kernel(
    where_ref, inv_hbm, res_hbm, act_t_hbm, codes_ref, grad_ref, taps_ref, small_ref,
    out_ref, taps_out_ref, bias_out_ref, inv_ref, res_ref, act_t_ref, dense, pre, grad_in, res_t, product, sems,
):
    sources = [inv_hbm, res_hbm, act_t_hbm]
    targets = [inv_ref, res_ref, act_t_ref]
    copies = [pltpu.make_async_copy(a, b, sems.at[n]) for n, (a, b) in enumerate(zip(sources, targets))]
    for copy in copies:
        copy.start()
    taps_out_ref[...] = small_ref[:TAPS, :]
    bias_out_ref[...] = small_ref[TAPS : TAPS + 1, :]
    tiles = CHUNK // 128
    for c in range(tiles):
        for b in range(2):
            pre[c, b, 0:8, :] = jnp.zeros((8, 128), F32)
            pre[c, b, 8 + 4 * TOK :, :] = jnp.zeros((8, 128), F32)
    keep = lax.broadcasted_iota(jnp.int32, (16, 128), 1) < SLOTS
    copies[0].wait()

    def expand(g, j, u):
        row = u * 16
        codes = codes_ref[j, row : row + 16, :].astype(F32)
        grad = grad_ref[j, row : row + 16, :].astype(F32)
        for side in range(2):
            if side:
                codes = pltpu.roll(codes, SLOTS, 1)
                grad = pltpu.roll(grad, SLOTS, 1)
            codes_side = jnp.where(keep, codes, 0.0)
            grad_side = jnp.where(keep, grad, 0.0)
            start = pl.multiple_of(j * TOK + side * 128 + row, 16)
            packed = inv_ref[pl.ds(start, 16), pl.ds(pl.multiple_of((g // 2) * 128, 128), 128)]
            into = pl.multiple_of(8 + (j // 2) * TOK + side * 128 + row, 8)
            for c in range(tiles):
                at = slice(c * 128, (c + 1) * 128)
                slot = slot_lane(packed, 7 * (lax.rem(g, 2) * 2 + c))
                wide = [
                    jnp.take_along_axis(codes_side[r : r + 8], slot[r : r + 8], axis=1)
                    for r in (0, 8)
                ]
                dense[pl.ds(start, 16), at] = jnp.concatenate(wide, axis=0).astype(BF16)
                for r in (0, 8):
                    pre[c, lax.rem(j, 2), pl.ds(into + r, 8), :] = jnp.take_along_axis(
                        grad_side[r : r + 8], slot[r : r + 8], axis=1
                    )

    def chunk(g, carry):
        lanes = pl.multiple_of(g * CHUNK, CHUNK)

        def expand_block(j, carry):
            for u in range(8):
                expand(g, j, u)
            return carry

        lax.fori_loop(0, GROUP, expand_block, 0)

        @pl.when(g == 0)
        def _():
            copies[1].wait()
            copies[2].wait()
            for j in range(GROUP):
                res_t[:, j * TOK : (j + 1) * TOK] = res_ref[j].T


        def spread(j, carry):
            into = pl.multiple_of(j * TOK, TOK)
            for c in range(tiles):
                taps = taps_ref[:, pl.ds(lanes + c * 128, 128)]
                for part in range(4):
                    row = (j // 2) * TOK + part * 64
                    total = jnp.zeros((64, 128), F32)
                    for k in range(TAPS):
                        total = (
                            total
                            + taps[k : k + 1]
                            * pre[c, lax.rem(j, 2), pl.ds(row + (8 + HALF - k), 64), :]
                        )
                    grad_in[pl.ds(into + part * 64, 64), c * 128 : (c + 1) * 128] = total.astype(
                        BF16
                    )
            return carry

        lax.fori_loop(0, GROUP, spread, 0)
        product[...] = jnp.dot(
            res_t[...], dense[...], preferred_element_type=F32
        ) + jnp.dot(act_t_ref[...], grad_in[...], preferred_element_type=F32)
        out_ref[:, pl.ds(lanes, CHUNK)] = product[pl.ds(pl.multiple_of(where_ref[0], 64), OWN), :]
        return carry

    lax.fori_loop(0, LATS // CHUNK, chunk, 0)


def dictionary_gradient(where, inv, res8, act_t, codes8, grad8, taps, small):
    return pl.pallas_call(
        dictionary_kernel,
        out_shape=(
            jax.ShapeDtypeStruct((OWN, LATS), F32),
            jax.ShapeDtypeStruct((TAPS, LATS), F32),
            jax.ShapeDtypeStruct((1, LATS), F32),
        ),
        in_specs=[pl.BlockSpec(memory_space=pltpu.SMEM)] + [ANY] * 3 + [VMEM] * 4,
        out_specs=(VMEM, VMEM, VMEM),
        scratch_shapes=[
            pltpu.VMEM((GROUP * TOK, 256), jnp.int32),
            pltpu.VMEM((GROUP, TOK, WIN), BF16),
            pltpu.VMEM((WIN, GROUP * TOK), BF16),
            pltpu.VMEM((GROUP * TOK, CHUNK), BF16),
            pltpu.VMEM((CHUNK // 128, 2, SEQ_ROWS, 128), F32),
            pltpu.VMEM((GROUP * TOK, CHUNK), BF16),
            pltpu.VMEM((WIN, GROUP * TOK), BF16),
            pltpu.VMEM((WIN, CHUNK), F32),
            pltpu.SemaphoreType.DMA((3,)),
        ],
        compiler_params=pltpu.CompilerParams(vmem_limit_bytes=LAST_MIB * 1024 * 1024),
        name="dictionary_gradient",
    )(where, inv, res8, act_t, codes8, grad8, taps, small)


def body(activations, dictionary, topk_ids, kernel_taps, enc_bias):
    act = activations[0]
    latents, part, dwin, lat, own_inv, ids8 = opening(
        act, dictionary, topk_ids[0].T, kernel_taps, enc_bias[None]
    )
    res8, act_t, inv = summed(part, act, ids8, own_inv)
    grad8, codes8, small = all_codes(latents, res8, dwin, ids8, own_inv, lat)
    where = (lax.axis_index("batch") * 64).astype(jnp.int32)[None]
    gradient, grad_taps, grad_bias = dictionary_gradient(
        where, inv, res8, act_t, codes8, grad8, kernel_taps, small
    )
    return gradient.T, grad_taps, grad_bias[0]


def solution(mesh):
    finer = Mesh(
        mesh.devices.reshape(mesh.shape["seq"], 2, 8, 2, mesh.shape["batch"]),
        ("seq", "lat_0", "lat_1", "lat_2", "batch"),
    )
    return jax.shard_map(
        body,
        mesh=finer,
        in_specs=(
            P("batch", "seq", None),
            P(LAT, None),
            P("batch", "seq", None),
            P(None, LAT),
            P(LAT),
        ),
        out_specs=(P(LAT, ("seq", "batch")), P(None, LAT), P(LAT)),
        check_vma=False,
    )
```
